256 devices in a mesh: grp: 4 (over x), dev: 64 (over z, y, core).
Axes of the slice: x: 4, y: 4, z: 8, core: 2. Of those that a mesh axis runs over, the one named last changes fastest.
Arguments:
- source_id: int32 [4194304], P(('grp', 'dev')), may hold values from 0 to 32767, as said below
- slot: int32 [4194304], P(('grp', 'dev')), may hold values from 0 to 127, as said below
- owner: int32 [32768], replicated, may hold values from 0 to 32767, as said below
- counts: int32 [32768], P(('grp', 'dev')), may hold values from 1 to 128, as said below
- partials: float32 [5, 4194304], P(None, ('grp', 'dev')), may hold values from -6 to 6
- residual: float32 [4194304], P(('grp', 'dev')), may hold values from -6 to 6
- weight: float32 [4194304], P(('grp', 'dev')), may hold values from 0.3 to 9
- prior: float32 [5, 32768], P(None, ('grp', 'dev')), may hold values from 0.5 to 4
Outputs:
- updates: float32 [5, 32768], P(None, ('grp', 'dev'))
- standardized: float32 [4194304], P(('grp', 'dev'))
- norm: float32 [], replicated
The draws below stay inside these ranges and needn't reach their ends.
Inputs may be any that keep to these rules, and one draw needn't show every extreme that they name: A permutation: source s stands at owner position owner[s], and position p belongs to device p // 128. `source_id`: the rows of one device stand in 256 aligned blocks of 64 rows; block k holds only rows whose source's owner position lies in device k's range. Over all rows, each pair of a source and a slot below 128 appears exactly once. A row is an observation when its slot is below its source's count, else padding. Each device's block of counts holds 128 at least once.
All inputs are finite; a program needn't handle non-finite values.
Results may differ from the reference program's by a relative error of at most 0.0003.
Values sent between devices are 32-bit elements; how exact they have to be, the bound alone decides.
A program may use at most 64 MiB of HBM per device.

```python
import math
import jax
import jax.numpy as jnp
from jax import lax

PARAMS = 5
PAD = 128
SRC_DEV = 128
SOURCES = 32768
ROWS_DEV = 16384
ROWS_ALL = 4194304
CAP = 64
N_GRP = 4
N_DEV = 64


def row_layout(key):
    base_key = jax.random.fold_in(key, 7001)
    devices_all = N_GRP * N_DEV
    placing = jax.random.permutation(jax.random.fold_in(base_key, 1), SOURCES).astype(jnp.int32)
    at_position = jnp.argsort(placing, stable=True).astype(jnp.int32)

    def owner_cells(owner_k):
        return jax.random.permutation(jax.random.fold_in(base_key, 1000 + owner_k), ROWS_DEV).astype(jnp.int32)
    cell_map = jax.vmap(owner_cells)(jnp.arange(devices_all, dtype=jnp.int32))
    cell_map = cell_map.reshape(devices_all, devices_all, CAP).transpose(1, 0, 2)
    owner_of = jnp.broadcast_to(jnp.arange(devices_all, dtype=jnp.int32)[None, :, None], cell_map.shape)
    position = owner_of * SRC_DEV + cell_map // PAD
    source_ids = at_position[position.reshape(-1)]
    slots = (cell_map % PAD).reshape(-1)
    return (placing, source_ids, slots)


def draw_owner(key, part):
    return row_layout(key)[0]


def draw_source_id(key, part):
    return row_layout(key)[1]


def draw_slot(key, part):
    return row_layout(key)[2]


def draw_counts(key, part):
    base_key = jax.random.fold_in(key, 7002)
    first_try = jax.random.randint(jax.random.fold_in(base_key, 1), (SOURCES,), 1, PAD + 1)
    second_try = jax.random.randint(jax.random.fold_in(base_key, 2), (SOURCES,), 1, PAD + 1)
    few_obs = jax.random.randint(jax.random.fold_in(base_key, 3), (SOURCES,), 1, PAD // 8 + 1)
    pick_low = jax.random.randint(jax.random.fold_in(base_key, 4), (SOURCES,), 0, 4) == 0
    result = jnp.where(pick_low, few_obs, jnp.maximum(first_try, second_try))
    full_slot = jax.random.randint(jax.random.fold_in(base_key, 5), (N_GRP * N_DEV,), 0, SRC_DEV)
    spots = jnp.arange(SOURCES, dtype=jnp.int32)
    result = jnp.where(spots % SRC_DEV == full_slot[spots // SRC_DEV], PAD, result)
    return result.astype(jnp.int32)


def draw_weight(key, part):
    row_device = jnp.arange(ROWS_ALL, dtype=jnp.int32) // ROWS_DEV
    rising = 1.0 + 2.0 * row_device.astype(jnp.float32) / max(N_GRP * N_DEV - 1, 1)
    spread = jnp.exp(jax.random.uniform(key, (ROWS_ALL,), jnp.float32, math.log(0.3), math.log(3.0)))
    return (spread * rising).astype(jnp.float32)


def steps_of(stream_key, shape, cuts, smallest, high):
    level, own = 1.0, jax.random.fold_in(stream_key, 6)
    for dim, blocks in cuts:
        heights = jnp.exp(jax.random.uniform(jax.random.fold_in(own, dim), (blocks,), jnp.float32, smallest / len(cuts), high / len(cuts)))
        level = level * jnp.repeat(heights, shape[dim] // blocks).reshape([-1 if axis == dim else 1 for axis in range(len(shape))])
    return level


def gaussian(own_key, extent, width, bound, pieces=(), kind=jnp.bfloat16):
    factor_of = steps_of(own_key, extent, pieces, -0.22, 0.18) if pieces else 1.0
    values = jax.random.normal(own_key, extent, jnp.float32) * width * factor_of
    return jnp.minimum(jnp.maximum(values, -bound), bound).astype(kind)


def setup_inputs(seed: int = 0) -> dict:
    streams_of = jax.random.split(jax.random.key(seed), 9)
    source_id = draw_source_id(jax.random.fold_in(streams_of[8], 71), 0)
    slot = draw_slot(jax.random.fold_in(streams_of[8], 71), 0)
    owner = draw_owner(jax.random.fold_in(streams_of[8], 71), 0)
    counts = draw_counts(jax.random.fold_in(streams_of[8], 71), 0)
    partials = gaussian(streams_of[4], (PARAMS, ROWS_ALL), 1.0, 6.0, ((1, 256),), jnp.float32)
    residual = gaussian(streams_of[5], (ROWS_ALL,), 1.0, 6.0, ((0, 256),), jnp.float32)
    weight = draw_weight(jax.random.fold_in(streams_of[8], 71), 0)
    prior = jnp.clip(jnp.exp(math.log(4.0) - 2.0794415 * jax.random.uniform(streams_of[7], (PARAMS, SOURCES), jnp.float32) ** steps_of(streams_of[7], (PARAMS, SOURCES), ((1, 256),), -0.2, 0.2)), 0.5, 4.0)
    return dict(source_id=source_id, slot=slot, owner=owner, counts=counts, partials=partials, residual=residual, weight=weight, prior=prior)


def solve_blocks(normal, moments):
    params = len(moments)
    factor = {}
    for column in range(params):
        running = normal[column][column]
        for earlier in range(column):
            running = running - factor[column, earlier] ** 2
        pivot_value = jnp.sqrt(running)
        factor[column, column] = pivot_value
        for target in range(column + 1, params):
            current = normal[target][column]
            for earlier in range(column):
                current = current - factor[target, earlier] * factor[column, earlier]
            factor[target, column] = current / pivot_value
    forward = []
    for target in range(params):
        current = moments[target]
        for earlier in range(target):
            current = current - factor[target, earlier] * forward[earlier]
        forward.append(current / factor[target, target])
    backward = [None] * params
    for target in reversed(range(params)):
        current = forward[target]
        for later in range(target + 1, params):
            current = current - factor[later, target] * backward[later]
        backward[target] = current / factor[target, target]
    return jnp.stack(backward)

def reference(source_id, slot, owner, counts, partials, residual, weight, prior):
    params = partials.shape[0]
    position = owner[source_id]
    live_mask = (slot < counts[position]).astype(jnp.float32)
    weighted = partials * (weight * live_mask)[None, :]
    normal = [[None] * params for _ in range(params)]
    for first_idx in range(params):
        for second_idx in range(first_idx, params):
            entry = jax.ops.segment_sum(weighted[first_idx] * partials[second_idx], position, num_segments=SOURCES)
            if first_idx == second_idx:
                entry = entry + prior[first_idx]
            normal[first_idx][second_idx] = entry
            normal[second_idx][first_idx] = entry
    moments = [jax.ops.segment_sum(weighted[first_idx] * residual, position, num_segments=SOURCES) for first_idx in range(params)]
    updates = solve_blocks(normal, moments)
    fitted = lax.optimization_barrier(jnp.sum(partials * updates[:, position], axis=0))
    fresh = (residual - fitted) * live_mask
    squares = jnp.sum(weight * fresh * fresh)
    live_total = jnp.sum(live_mask)
    norm = jnp.sqrt(squares / live_total + 1e-06)
    return (updates, fresh * jnp.sqrt(weight) / norm, norm)
```

```python
import functools

import jax
import jax.numpy as jnp
from jax import lax
from jax.experimental import pallas as pl
from jax.experimental.pallas import tpu as pltpu
from jax.sharding import PartitionSpec as P

MESH = pl.DeviceIdType.MESH
F32 = jnp.float32
BF16 = jnp.bfloat16
LANES = 128
ROWS_Y = 4
CORES = 2
PARAMS = 5
GROUP = 16


def split_bf16(value):
    high = value.astype(BF16).astype(F32)
    rest = value - high
    middle = rest.astype(BF16).astype(F32)
    return high, middle, rest - middle


def column_of(row):
    square = (LANES, LANES)
    diagonal = lax.broadcasted_iota(jnp.int32, square, 0) == lax.broadcasted_iota(jnp.int32, square, 1)
    return jnp.sum(jnp.where(diagonal, jnp.broadcast_to(row, square), 0.0), axis=1, keepdims=True)


def solve_blocks(normal, moments):
    params = len(moments)
    factor = {}
    for column in range(params):
        running = normal[column][column]
        for earlier in range(column):
            running = running - factor[column, earlier] ** 2
        pivot_value = jnp.sqrt(running)
        factor[column, column] = pivot_value
        for target in range(column + 1, params):
            current = normal[target][column]
            for earlier in range(column):
                current = current - factor[target, earlier] * factor[column, earlier]
            factor[target, column] = current / pivot_value
    forward = []
    for target in range(params):
        current = moments[target]
        for earlier in range(target):
            current = current - factor[target, earlier] * forward[earlier]
        forward.append(current / factor[target, target])
    backward = [None] * params
    for target in reversed(range(params)):
        current = forward[target]
        for later in range(target + 1, params):
            current = current - factor[later, target] * backward[later]
        backward[target] = current / factor[target, target]
    return backward


def kernel(
    shape,
    source_ref,
    slot_ref,
    owner_ref,
    counts_ref,
    partials_ref,
    residual_ref,
    weight_ref,
    prior_ref,
    updates_ref,
    standard_ref,
    norm_ref,
    send_buf,
    recv_buf,
    halves,
    onehot,
    stats,
    total,
    table,
    facts,
    sums,
    other_sums,
    update_rows,
    fresh_out,
    fresh_in,
    square_out,
    square_in,
    square_total,
    send_sem,
    recv_sem,
    pair_send,
    pair_recv,
    back_send,
    back_recv,
):
    size_x, size_y, size_z = shape
    chips = size_x * size_y * size_z
    groups = chips // GROUP
    me_x = lax.axis_index("grp")
    me_dev = lax.axis_index("dev")
    core = me_dev % CORES
    me_y = (me_dev // CORES) % size_y
    me_z = me_dev // (CORES * size_y)
    me_chip = (me_x * size_z + me_z) * size_y + me_y

    def offset(p):
        q = p // GROUP
        inside = GROUP - 1 - p % GROUP
        dz = (size_z // 2 + ((q + 1) // 2) * (1 - 2 * (q % 2))) % size_z
        return inside // size_y, inside % size_y, dz

    def place(x, y, z):
        return (x, (z * size_y + y) * CORES + core), (x * size_z + z) * size_y + y

    def ahead(p):
        dx, dy, dz = offset(p)
        return place((me_x + dx) % size_x, (me_y + dy) % size_y, (me_z + dz) % size_z)

    def behind(p):
        dx, dy, dz = offset(p)
        return place(
            (me_x + size_x - dx) % size_x,
            (me_y + size_y - dy) % size_y,
            (me_z + size_z - dz) % size_z,
        )

    partner = (me_x, me_dev + 1 - 2 * core)
    barrier = pltpu.get_barrier_semaphore()

    def greet(p, carry):
        device, _ = ahead(p)
        pl.semaphore_signal(barrier, inc=1, device_id=device, device_id_type=MESH)
        return carry

    pl.semaphore_signal(barrier, inc=1, device_id=partner, device_id_type=MESH)
    lax.fori_loop(0, chips - 1, greet, 0)

    for block in range(chips // 8):
        rows = pl.ds(block * 8, 8)
        cell = (source_ref[rows, :] * LANES + slot_ref[rows, :]).astype(F32)
        send_buf[pl.ds(block * 64 + PARAMS, 8, stride=8), :] = residual_ref[rows, :]
        send_buf[pl.ds(block * 64 + PARAMS + 1, 8, stride=8), :] = weight_ref[rows, :]
        send_buf[pl.ds(block * 64 + PARAMS + 2, 8, stride=8), :] = cell
        for tile in range(block * 8, block * 8 + 8):
            send_buf[tile * 8 : tile * 8 + PARAMS, :] = partials_ref[:, tile * LANES : (tile + 1) * LANES]
    facts[pl.ds(pl.multiple_of(core * 8, 8), 8), :] = jnp.concatenate(
        [prior_ref[...], counts_ref[...].astype(F32), jnp.zeros((2, LANES), F32)], axis=0
    )

    sublane = lax.broadcasted_iota(jnp.int32, (LANES, LANES), 0)
    lane = lax.broadcasted_iota(jnp.int32, (1, LANES), 1)
    for side in range(CORES):
        base = (me_chip * CORES + side) * LANES

        def look(step, found):
            rows = owner_ref[pl.ds(pl.multiple_of(step * 8, 8), 8), :] - base
            for row in range(8):
                here = lane + (step * 8 + row) * LANES
                found = jnp.where(rows[row : row + 1, :] == sublane, here, found)
            return found

        found = lax.fori_loop(0, owner_ref.shape[0] // 8, look, jnp.zeros((LANES, LANES), jnp.int32))
        first = jnp.sum(found.astype(F32), axis=1, keepdims=True) * LANES
        table[side, 0] = jnp.broadcast_to(first, (LANES, LANES))

    pl.semaphore_wait(barrier, chips)

    facts_copy = pltpu.make_async_remote_copy(
        src_ref=facts.at[pl.ds(pl.multiple_of(core * 8, 8), 8), :],
        dst_ref=facts.at[pl.ds(pl.multiple_of(core * 8, 8), 8), :],
        send_sem=pair_send.at[0],
        recv_sem=pair_recv.at[0],
        device_id=partner,
        device_id_type=MESH,
    )
    facts_copy.start()

    def tile_copy(p):
        device, chip = ahead(p)
        return pltpu.make_async_remote_copy(
            src_ref=send_buf.at[pl.ds(pl.multiple_of(chip * 8, 8), 8), :],
            dst_ref=recv_buf.at[pl.ds(pl.multiple_of(p * 8, 8), 8), :],
            send_sem=send_sem,
            recv_sem=recv_sem.at[p // GROUP],
            device_id=device,
            device_id_type=MESH,
        )

    def send_tile(p, carry):
        tile_copy(p).start()
        return carry

    lax.fori_loop(0, chips - 1, send_tile, 0)
    recv_buf[(chips - 1) * 8 : chips * 8, :] = send_buf[pl.ds(pl.multiple_of(me_chip * 8, 8), 8), :]

    facts_copy.wait()
    for side in range(CORES):
        count = column_of(facts[side * 8 + PARAMS : side * 8 + PARAMS + 1, :])
        table[side, 0] = table[side, 0] + (count - 1.0) * 0.5
        table[side, 1] = jnp.broadcast_to(count * 0.5, (LANES, LANES))

    def wait_rows(source, target, count, send, recv, to):
        return pltpu.make_async_remote_copy(
            src_ref=source.at[pl.ds(0, count)],
            dst_ref=target.at[pl.ds(0, count)],
            send_sem=send,
            recv_sem=recv,
            device_id=to,
            device_id_type=MESH,
        )

    low = lax.broadcasted_iota(jnp.int32, (8, LANES), 1) < LANES // 2
    total[...] = jnp.zeros_like(total)

    def gather_group(q):
        def pair(v, carry):
            start = pl.multiple_of(q * GROUP * 8 + v * 16, 16)
            even = recv_buf[pl.ds(start, 8), :]
            odd = recv_buf[pl.ds(start + 8, 8), :]
            left = jnp.where(low, even, pltpu.roll(odd, LANES // 2, 1))
            right = jnp.where(low, pltpu.roll(even, LANES // 2, 1), odd)
            for side, rows in ((0, left), (1, right)):
                halves[side, pl.ds(pl.multiple_of(q * GROUP * 4 + v * 8, 8), 8), :] = rows
                inside = jnp.abs(rows[7:8, :] - table[side, 0]) < table[side, 1]
                where = pl.ds(pl.multiple_of((q * (GROUP // 2) + v) * LANES, LANES), LANES)
                onehot[side, :, where] = jnp.where(inside, 1.0, 0.0).astype(BF16)
                weighted = rows * rows[6:7, :]
                terms = jnp.concatenate([weighted[i : i + 1, :] * rows for i in range(PARAMS)], axis=0)
                parts = jnp.concatenate([*split_bf16(terms), jnp.zeros((8, LANES), F32)], axis=0)
                stats[side, :, pl.ds(pl.multiple_of(v * LANES, LANES), LANES)] = parts.astype(BF16)
            return carry

        for v in range(GROUP // 2):
            pair(v, 0)
        for side in range(CORES):
            where = pl.ds(pl.multiple_of(q * (GROUP // 2) * LANES, LANES), (GROUP // 2) * LANES)
            total[side] += lax.dot_general(
                stats[side], onehot[side, :, where], (((1,), (1,)), ((), ())), preferred_element_type=F32
            )

    def arrive(q, carry):
        wait_rows(send_buf, recv_buf, GROUP * 8, send_sem, recv_sem.at[q], partner).wait_recv()
        gather_group(q)
        return carry

    lax.fori_loop(0, groups - 1, arrive, 0)
    wait_rows(send_buf, recv_buf, (GROUP - 1) * 8, send_sem, recv_sem.at[groups - 1], partner).wait_recv()
    gather_group(groups - 1)

    span = PARAMS * 8
    for side in range(CORES):
        sums[side * span : (side + 1) * span, :] = (
            total[side, 0:span, :] + total[side, span : 2 * span, :] + total[side, 2 * span : 3 * span, :]
        )
    sums_copy = pltpu.make_async_remote_copy(
        src_ref=sums,
        dst_ref=other_sums,
        send_sem=pair_send.at[1],
        recv_sem=pair_recv.at[1],
        device_id=partner,
        device_id_type=MESH,
    )
    sums_copy.start()
    sums_copy.wait_recv()

    def summed(row):
        rows = pl.ds(row, CORES, stride=span)
        return sums[rows, :] + other_sums[rows, :]

    normal = [[None] * PARAMS for _ in range(PARAMS)]
    for i in range(PARAMS):
        for j in range(i, PARAMS):
            entry = summed(i * 8 + j)
            if i == j:
                entry = entry + facts[pl.ds(i, CORES, stride=8), :]
            normal[i][j] = entry
            normal[j][i] = entry
    moments = [summed(i * 8 + PARAMS) for i in range(PARAMS)]
    updates = solve_blocks(normal, moments)
    for i in range(PARAMS):
        update_rows[pl.ds(i, CORES, stride=8), :] = updates[i]
    update_rows[pl.ds(PARAMS, CORES, stride=8), :] = jnp.full((CORES, LANES), -1.0, F32)
    for row in (PARAMS + 1, PARAMS + 2):
        update_rows[pl.ds(row, CORES, stride=8), :] = jnp.zeros((CORES, LANES), F32)
    updates_ref[...] = update_rows[pl.ds(pl.multiple_of(core * 8, 8), 8), :][0:PARAMS, :]

    spread = []
    for side in range(CORES):
        parts = split_bf16(update_rows[side * 8 : side * 8 + 8, :])
        spread.append(jnp.concatenate([*parts, jnp.zeros((8, LANES), F32)], axis=0).astype(BF16))

    square_total[...] = jnp.zeros_like(square_total)

    def refit_group(q):
        fitted = []
        for side in range(CORES):
            where = pl.ds(pl.multiple_of(q * (GROUP // 2) * LANES, LANES), (GROUP // 2) * LANES)
            got = lax.dot_general(
                spread[side], onehot[side, :, where], (((1,), (0,)), ((), ())), preferred_element_type=F32
            )
            fitted.append(got[0:8, :] + got[8:16, :] + got[16:24, :])
        squares = square_total[...]
        for v in range(GROUP // 2):
            fresh = []
            for side in range(CORES):
                rows = halves[side, pl.ds(pl.multiple_of(q * GROUP * 4 + v * 8, 8), 8), :]
                term = rows * fitted[side][:, v * LANES : (v + 1) * LANES]
                line = -jnp.sum(term, axis=0, keepdims=True)
                squares = squares + rows[6:7, :] * line * line
                fresh.append(line)
            left, right = fresh
            at = q * GROUP + v * 2
            fresh_out[at] = jnp.where(low[0:1], left, pltpu.roll(right, LANES // 2, 1))
            fresh_out[at + 1] = jnp.where(low[0:1], pltpu.roll(left, LANES // 2, 1), right)
        square_total[...] = squares

    def fresh_copy(p):
        device, _ = behind(p)
        return pltpu.make_async_remote_copy(
            src_ref=fresh_out.at[p],
            dst_ref=fresh_in.at[me_chip],
            send_sem=back_send.at[0],
            recv_sem=back_recv.at[0],
            device_id=device,
            device_id_type=MESH,
        )

    def square_copy(p):
        device, _ = behind(p)
        return pltpu.make_async_remote_copy(
            src_ref=square_out.at[0],
            dst_ref=square_in.at[me_chip],
            send_sem=back_send.at[1],
            recv_sem=back_recv.at[1],
            device_id=device,
            device_id_type=MESH,
        )

    def send_fresh(p, carry):
        fresh_copy(p).start()
        return carry

    def send_square(p, carry):
        square_copy(p).start()
        return carry

    def leave(q, carry):
        refit_group(q)
        lax.fori_loop(q * GROUP, q * GROUP + GROUP, send_fresh, 0)
        return carry

    lax.fori_loop(0, groups - 1, leave, 0)
    refit_group(groups - 1)
    lax.fori_loop((groups - 1) * GROUP, chips - 1, send_fresh, 0)

    squares = square_total[...]
    count_row = counts_ref[...].astype(F32)
    squares = squares + pltpu.roll(squares, LANES // 2, 1)
    count_row = count_row + pltpu.roll(count_row, LANES // 2, 1)
    square_row = jnp.where(low[0:1], squares, count_row)
    square_out[0] = square_row
    lax.fori_loop(0, chips - 1, send_square, 0)
    square_in[me_chip] = square_row
    fresh_in[me_chip] = fresh_out[chips - 1]

    wait_rows(square_in, square_in, chips - 1, back_send.at[1], back_recv.at[1], partner).wait_recv()
    square_total[...] = jnp.sum(square_in[...], axis=0)
    last_copy = pltpu.make_async_remote_copy(
        src_ref=square_total,
        dst_ref=square_out.at[1],
        send_sem=pair_send.at[2],
        recv_sem=pair_recv.at[2],
        device_id=partner,
        device_id_type=MESH,
    )
    last_copy.start()
    wait_rows(fresh_in, fresh_in, chips - 1, back_send.at[0], back_recv.at[0], partner).wait_recv()
    last_copy.wait_recv()
    whole = square_total[...] + square_out[1]
    square_sum = jnp.sum(jnp.where(low[0:1], whole, 0.0), axis=1, keepdims=True)
    count_sum = jnp.sum(jnp.where(low[0:1], 0.0, whole), axis=1, keepdims=True)
    norm = jnp.sqrt(square_sum / count_sum + 1e-6)
    norm_ref[...] = jnp.broadcast_to(norm, (1, LANES))
    standard_ref[...] = jnp.reshape(fresh_in[...], (chips, LANES)) * jnp.sqrt(weight_ref[...]) / norm

    wait_rows(send_buf, recv_buf, (chips - 1) * 8, send_sem, send_sem, partner).wait_send()
    sums_copy.wait_send()
    last_copy.wait_send()
    wait_rows(fresh_in, fresh_in, chips - 1, back_send.at[0], back_recv.at[0], partner).wait_send()
    wait_rows(square_in, square_in, chips - 1, back_send.at[1], back_recv.at[1], partner).wait_send()


def body(shape, source_id, slot, owner, counts, partials, residual, weight, prior):
    size_x, size_y, size_z = shape
    chips = size_x * size_y * size_z
    groups = chips // GROUP
    square = (chips, LANES)
    vmem = pl.BlockSpec(memory_space=pltpu.VMEM)
    updates, standard, norm = pl.pallas_call(
        functools.partial(kernel, shape),
        out_shape=(
            jax.ShapeDtypeStruct((PARAMS, LANES), F32),
            jax.ShapeDtypeStruct(square, F32),
            jax.ShapeDtypeStruct((1, LANES), F32),
        ),
        in_specs=[vmem] * 8,
        out_specs=(vmem, vmem, vmem),
        scratch_shapes=[
            pltpu.VMEM((chips * 8, LANES), F32),
            pltpu.VMEM((chips * 8, LANES), F32),
            pltpu.VMEM((CORES, chips * 4, LANES), F32),
            pltpu.VMEM((CORES, LANES, chips * LANES // 2), BF16),
            pltpu.VMEM((CORES, LANES, GROUP // 2 * LANES), BF16),
            pltpu.VMEM((CORES, LANES, LANES), F32),
            pltpu.VMEM((CORES, 2, LANES, LANES), F32),
            pltpu.VMEM((CORES * 8, LANES), F32),
            pltpu.VMEM((CORES * PARAMS * 8, LANES), F32),
            pltpu.VMEM((CORES * PARAMS * 8, LANES), F32),
            pltpu.VMEM((CORES * 8, LANES), F32),
            pltpu.VMEM((chips, 1, LANES), F32),
            pltpu.VMEM((chips, 1, LANES), F32),
            pltpu.VMEM((2, 1, LANES), F32),
            pltpu.VMEM((chips, 1, LANES), F32),
            pltpu.VMEM((1, LANES), F32),
            pltpu.SemaphoreType.DMA,
            pltpu.SemaphoreType.DMA((groups,)),
            pltpu.SemaphoreType.DMA((3,)),
            pltpu.SemaphoreType.DMA((3,)),
            pltpu.SemaphoreType.DMA((2,)),
            pltpu.SemaphoreType.DMA((2,)),
        ],
        compiler_params=pltpu.CompilerParams(collective_id=0, has_side_effects=True),
    )(
        source_id.reshape(square),
        slot.reshape(square),
        owner.reshape(-1, LANES),
        counts.reshape(1, LANES),
        partials,
        residual.reshape(square),
        weight.reshape(square),
        prior,
    )
    return updates, standard.reshape(-1), norm[0, 0]


def solution(mesh):
    shape = (mesh.shape["grp"], ROWS_Y, mesh.shape["dev"] // (ROWS_Y * CORES))
    rows = P(("grp", "dev"))
    columns = P(None, ("grp", "dev"))
    in_specs = (rows, rows, P(), rows, columns, rows, rows, columns)
    out_specs = (columns, rows, P())
    return jax.shard_map(
        functools.partial(body, shape), mesh=mesh, in_specs=in_specs, out_specs=out_specs, check_vma=False
    )
```

```python
import functools

import jax
import jax.numpy as jnp
from jax import lax
from jax.experimental import pallas as pl
from jax.experimental.pallas import tpu as pltpu
from jax.sharding import PartitionSpec as P

MESH = pl.DeviceIdType.MESH
F32 = jnp.float32
BF16 = jnp.bfloat16
LANES = 128
ROWS_Y = 4
CORES = 2
PARAMS = 5
FIELDS = 7
GROUP = 16


def split_bf16(value):
    high = value.astype(BF16).astype(F32)
    rest = value - high
    middle = rest.astype(BF16).astype(F32)
    return high, middle, rest - middle


def column_of(row):
    square = (LANES, LANES)
    diagonal = lax.broadcasted_iota(jnp.int32, square, 0) == lax.broadcasted_iota(jnp.int32, square, 1)
    return jnp.sum(jnp.where(diagonal, jnp.broadcast_to(row, square), 0.0), axis=1, keepdims=True)


def solve_blocks(normal, moments):
    params = len(moments)
    factor = {}
    for column in range(params):
        running = normal[column][column]
        for earlier in range(column):
            running = running - factor[column, earlier] ** 2
        pivot_value = jnp.sqrt(running)
        factor[column, column] = pivot_value
        for target in range(column + 1, params):
            current = normal[target][column]
            for earlier in range(column):
                current = current - factor[target, earlier] * factor[column, earlier]
            factor[target, column] = current / pivot_value
    forward = []
    for target in range(params):
        current = moments[target]
        for earlier in range(target):
            current = current - factor[target, earlier] * forward[earlier]
        forward.append(current / factor[target, target])
    backward = [None] * params
    for target in reversed(range(params)):
        current = forward[target]
        for later in range(target + 1, params):
            current = current - factor[later, target] * backward[later]
        backward[target] = current / factor[target, target]
    return backward


def kernel(
    shape,
    *refs,
):
    inputs, (updates_ref, standard_ref, norm_ref) = refs[0:8], refs[8:11]
    loaded = refs[11:19]
    (send_buf, recv_buf, halves, onehot, stats, total, table, facts, sums, other_sums) = refs[19:29]
    (update_rows, fresh_out, fresh_in, square_out, square_in, square_total) = refs[29:35]
    (load_sem, send_sem, recv_sem, pair_send, pair_recv, back_send, back_recv) = refs[35:42]
    size_x, size_y, size_z = shape
    chips = size_x * size_y * size_z
    groups = chips // GROUP
    me_x = lax.axis_index("grp")
    me_dev = lax.axis_index("dev")
    core = me_dev % CORES
    me_y = (me_dev // CORES) % size_y
    me_z = me_dev // (CORES * size_y)
    me_chip = (me_x * size_z + me_z) * size_y + me_y

    xs = [(me_x + dx) % size_x for dx in range(size_x)]
    ys = [(me_y + dy) % size_y for dy in range(size_y)]

    def group_z(q):
        return (size_z // 2 + ((q + 1) // 2) * (1 - 2 * (q % 2))) % size_z

    def in_group(q, count, forward, action):
        dz = group_z(q)
        z = (me_z + dz) % size_z if forward else (me_z + size_z - dz) % size_z
        for slot in range(count):
            inside = GROUP - 1 - slot
            dx, dy = inside // size_y, inside % size_y
            if not forward:
                dx, dy = (size_x - dx) % size_x, (size_y - dy) % size_y
            x, y = xs[dx], ys[dy]
            action(q, slot, (x, (z * size_y + y) * CORES + core), (x * size_z + z) * size_y + y)

    def everywhere(forward, action):
        def one(q, carry):
            in_group(q, GROUP, forward, action)
            return carry

        lax.fori_loop(0, groups - 1, one, 0)
        in_group(groups - 1, GROUP - 1, forward, action)

    partner = (me_x, me_dev + 1 - 2 * core)
    barrier = pltpu.get_barrier_semaphore()

    for block in range(chips // 8):
        recv_buf[pl.ds(block * 64 + FIELDS, 8, stride=8), :] = jnp.zeros((8, LANES), F32)

    pl.semaphore_signal(barrier, inc=1, device_id=partner, device_id_type=MESH)
    everywhere(
        True,
        lambda q, slot, device, chip: pl.semaphore_signal(barrier, inc=1, device_id=device, device_id_type=MESH),
    )

    loads = [
        pltpu.make_async_copy(source, target, load_sem.at[index])
        for index, (source, target) in enumerate(zip(inputs, loaded, strict=True))
    ]
    for load in loads:
        load.start()
    source_ref, slot_ref, owner_ref, counts_ref, partials_ref, residual_ref, weight_ref, prior_ref = loaded
    for load in loads:
        load.wait()

    for block in range(chips // 8):
        rows = pl.ds(block * 8, 8)
        root = jnp.sqrt(weight_ref[rows, :])
        cell = (source_ref[rows, :] * LANES + slot_ref[rows, :]).astype(F32)
        send_buf[pl.ds(block * 64 + PARAMS, 8, stride=8), :] = residual_ref[rows, :] * root
        send_buf[pl.ds(block * 64 + PARAMS + 1, 8, stride=8), :] = cell
        for row in range(8):
            tile = block * 8 + row
            send_buf[tile * 8 : tile * 8 + PARAMS, :] = (
                partials_ref[:, tile * LANES : (tile + 1) * LANES] * root[row : row + 1, :]
            )
    facts[pl.ds(pl.multiple_of(core * 8, 8), 8), :] = jnp.concatenate(
        [prior_ref[...], counts_ref[...].astype(F32), jnp.zeros((2, LANES), F32)], axis=0
    )

    pl.semaphore_wait(barrier, chips)

    facts_copy = pltpu.make_async_remote_copy(
        src_ref=facts.at[pl.ds(pl.multiple_of(core * 8, 8), 8), :],
        dst_ref=facts.at[pl.ds(pl.multiple_of(core * 8, 8), 8), :],
        send_sem=pair_send.at[0],
        recv_sem=pair_recv.at[0],
        device_id=partner,
        device_id_type=MESH,
    )
    facts_copy.start()

    def send_tile(q, slot, device, chip):
        pltpu.make_async_remote_copy(
            src_ref=send_buf.at[pl.ds(pl.multiple_of(chip * 8, 8), FIELDS), :],
            dst_ref=recv_buf.at[pl.ds(pl.multiple_of(q * (GROUP * 8), 8) + slot * 8, FIELDS), :],
            send_sem=send_sem,
            recv_sem=recv_sem.at[q],
            device_id=device,
            device_id_type=MESH,
        ).start()

    everywhere(True, send_tile)
    recv_buf[(chips - 1) * 8 : chips * 8 - 1, :] = send_buf[pl.ds(pl.multiple_of(me_chip * 8, 8), 8), :][0:FIELDS, :]

    sublane = lax.broadcasted_iota(jnp.int32, (LANES, LANES), 0)
    lane = lax.broadcasted_iota(jnp.int32, (1, LANES), 1)
    for side in range(CORES):
        base = (me_chip * CORES + side) * LANES

        def look(step, found):
            rows = owner_ref[pl.ds(pl.multiple_of(step * 8, 8), 8), :] - base
            for row in range(8):
                here = lane + (step * 8 + row) * LANES
                found = jnp.where(rows[row : row + 1, :] == sublane, here, found)
            return found

        found = lax.fori_loop(0, owner_ref.shape[0] // 8, look, jnp.zeros((LANES, LANES), jnp.int32))
        first = jnp.sum(found.astype(F32), axis=1, keepdims=True) * LANES
        table[side, 0] = jnp.broadcast_to(first, (LANES, LANES))

    facts_copy.wait()
    for side in range(CORES):
        count = column_of(facts[side * 8 + PARAMS : side * 8 + PARAMS + 1, :])
        table[side, 0] = table[side, 0] + (count - 1.0) * 0.5
        table[side, 1] = jnp.broadcast_to(count * 0.5, (LANES, LANES))

    def wait_rows(source, target, count, send, recv, to):
        return pltpu.make_async_remote_copy(
            src_ref=source.at[pl.ds(0, count)],
            dst_ref=target.at[pl.ds(0, count)],
            send_sem=send,
            recv_sem=recv,
            device_id=to,
            device_id_type=MESH,
        )

    low = lax.broadcasted_iota(jnp.int32, (8, LANES), 1) < LANES // 2
    total[...] = jnp.zeros_like(total)

    def gather_group(q):
        def pair(v, carry):
            start = pl.multiple_of(q * GROUP * 8 + v * 16, 16)
            even = recv_buf[pl.ds(start, 8), :]
            odd = recv_buf[pl.ds(start + 8, 8), :]
            left = jnp.where(low, even, pltpu.roll(odd, LANES // 2, 1))
            right = jnp.where(low, pltpu.roll(even, LANES // 2, 1), odd)
            for side, rows in ((0, left), (1, right)):
                halves[side, pl.ds(pl.multiple_of(q * GROUP * 4 + v * 8, 8), 8), :] = rows
                inside = jnp.abs(rows[6:7, :] - table[side, 0]) < table[side, 1]
                where = pl.ds(pl.multiple_of((q * (GROUP // 2) + v) * LANES, LANES), LANES)
                onehot[side, :, where] = jnp.where(inside, 1.0, 0.0).astype(BF16)
                terms = jnp.concatenate([rows[i : i + 1, :] * rows for i in range(PARAMS)], axis=0)
                parts = jnp.concatenate([*split_bf16(terms), jnp.zeros((8, LANES), F32)], axis=0)
                stats[side, :, pl.ds(pl.multiple_of(v * LANES, LANES), LANES)] = parts.astype(BF16)
            return carry

        for v in range(GROUP // 2):
            pair(v, 0)
        for side in range(CORES):
            where = pl.ds(pl.multiple_of(q * (GROUP // 2) * LANES, LANES), (GROUP // 2) * LANES)
            total[side] += lax.dot_general(
                stats[side], onehot[side, :, where], (((1,), (1,)), ((), ())), preferred_element_type=F32
            )

    def arrive(q, carry):
        wait_rows(send_buf, recv_buf, GROUP * FIELDS, send_sem, recv_sem.at[q], partner).wait_recv()
        gather_group(q)
        return carry

    lax.fori_loop(0, groups - 1, arrive, 0)
    wait_rows(send_buf, recv_buf, (GROUP - 1) * FIELDS, send_sem, recv_sem.at[groups - 1], partner).wait_recv()
    gather_group(groups - 1)

    span = PARAMS * 8
    for side in range(CORES):
        sums[side * span : (side + 1) * span, :] = (
            total[side, 0:span, :] + total[side, span : 2 * span, :] + total[side, 2 * span : 3 * span, :]
        )
    sums_copy = pltpu.make_async_remote_copy(
        src_ref=sums,
        dst_ref=other_sums,
        send_sem=pair_send.at[1],
        recv_sem=pair_recv.at[1],
        device_id=partner,
        device_id_type=MESH,
    )
    sums_copy.start()
    sums_copy.wait_recv()

    def summed(row):
        rows = pl.ds(row, CORES, stride=span)
        return sums[rows, :] + other_sums[rows, :]

    normal = [[None] * PARAMS for _ in range(PARAMS)]
    for i in range(PARAMS):
        for j in range(i, PARAMS):
            entry = summed(i * 8 + j)
            if i == j:
                entry = entry + facts[pl.ds(i, CORES, stride=8), :]
            normal[i][j] = entry
            normal[j][i] = entry
    moments = [summed(i * 8 + PARAMS) for i in range(PARAMS)]
    updates = solve_blocks(normal, moments)
    for i in range(PARAMS):
        update_rows[pl.ds(i, CORES, stride=8), :] = updates[i]
    update_rows[pl.ds(PARAMS, CORES, stride=8), :] = jnp.full((CORES, LANES), -1.0, F32)
    for row in (PARAMS + 1, PARAMS + 2):
        update_rows[pl.ds(row, CORES, stride=8), :] = jnp.zeros((CORES, LANES), F32)
    updates_ref[...] = update_rows[pl.ds(pl.multiple_of(core * 8, 8), 8), :][0:PARAMS, :]

    spread = []
    for side in range(CORES):
        parts = split_bf16(update_rows[side * 8 : side * 8 + 8, :])
        spread.append(jnp.concatenate([*parts, jnp.zeros((8, LANES), F32)], axis=0).astype(BF16))

    square_total[...] = jnp.zeros_like(square_total)

    def refit_group(q):
        fitted = []
        for side in range(CORES):
            where = pl.ds(pl.multiple_of(q * (GROUP // 2) * LANES, LANES), (GROUP // 2) * LANES)
            got = lax.dot_general(
                spread[side], onehot[side, :, where], (((1,), (0,)), ((), ())), preferred_element_type=F32
            )
            fitted.append(got[0:8, :] + got[8:16, :] + got[16:24, :])
        squares = square_total[...]
        for v in range(GROUP // 2):
            fresh = []
            for side in range(CORES):
                rows = halves[side, pl.ds(pl.multiple_of(q * GROUP * 4 + v * 8, 8), 8), :]
                term = rows * fitted[side][:, v * LANES : (v + 1) * LANES]
                line = -jnp.sum(term, axis=0, keepdims=True)
                squares = squares + line * line
                fresh.append(line)
            left, right = fresh
            at = q * GROUP + v * 2
            fresh_out[at] = jnp.where(low[0:1], left, pltpu.roll(right, LANES // 2, 1))
            fresh_out[at + 1] = jnp.where(low[0:1], pltpu.roll(left, LANES // 2, 1), right)
        square_total[...] = squares

    def send_fresh(q, slot, device, chip):
        pltpu.make_async_remote_copy(
            src_ref=fresh_out.at[q * GROUP + slot],
            dst_ref=fresh_in.at[me_chip],
            send_sem=back_send.at[0],
            recv_sem=back_recv.at[0],
            device_id=device,
            device_id_type=MESH,
        ).start()

    def send_square(q, slot, device, chip):
        pltpu.make_async_remote_copy(
            src_ref=square_out.at[2],
            dst_ref=square_in.at[me_chip],
            send_sem=back_send.at[1],
            recv_sem=back_recv.at[1],
            device_id=device,
            device_id_type=MESH,
        ).start()

    def leave(q, carry):
        refit_group(q)
        in_group(q, GROUP, False, send_fresh)
        return carry

    lax.fori_loop(0, groups - 1, leave, 0)
    refit_group(groups - 1)

    squares = square_total[...]
    count_row = counts_ref[...].astype(F32)
    squares = squares + pltpu.roll(squares, LANES // 2, 1)
    count_row = count_row + pltpu.roll(count_row, LANES // 2, 1)
    square_out[0] = jnp.where(low[0:1], squares, count_row)
    square_copy = pltpu.make_async_remote_copy(
        src_ref=square_out.at[0],
        dst_ref=square_out.at[1],
        send_sem=pair_send.at[2],
        recv_sem=pair_recv.at[2],
        device_id=partner,
        device_id_type=MESH,
    )
    square_copy.start()
    in_group(groups - 1, GROUP - 1, False, send_fresh)
    square_copy.wait_recv()
    square_row = square_out[0] + square_out[1]
    square_out[2] = square_row
    everywhere(False, send_square)
    square_in[me_chip] = square_row
    fresh_in[me_chip] = fresh_out[chips - 1]
    wait_rows(fresh_in, fresh_in, chips - 1, back_send.at[0], back_recv.at[0], partner).wait_recv()
    wait_rows(square_in, square_in, chips - 1, back_send.at[1], back_recv.at[1], partner).wait_recv()
    whole = jnp.sum(square_in[...], axis=0)
    square_sum = jnp.sum(jnp.where(low[0:1], whole, 0.0), axis=1, keepdims=True)
    count_sum = jnp.sum(jnp.where(low[0:1], 0.0, whole), axis=1, keepdims=True)
    norm = jnp.sqrt(square_sum / count_sum + 1e-6)
    norm_ref[...] = jnp.broadcast_to(norm, (1, LANES))
    standard_ref[...] = jnp.reshape(fresh_in[...], (chips, LANES)) / norm

    wait_rows(send_buf, recv_buf, (chips - 1) * FIELDS, send_sem, send_sem, partner).wait_send()
    sums_copy.wait_send()
    square_copy.wait_send()
    wait_rows(fresh_in, fresh_in, chips - 1, back_send.at[0], back_recv.at[0], partner).wait_send()
    wait_rows(square_in, square_in, chips - 1, back_send.at[1], back_recv.at[1], partner).wait_send()


def body(shape, source_id, slot, owner, counts, partials, residual, weight, prior):
    size_x, size_y, size_z = shape
    chips = size_x * size_y * size_z
    groups = chips // GROUP
    square = (chips, LANES)
    arrays = (
        source_id.reshape(square),
        slot.reshape(square),
        owner.reshape(-1, LANES),
        counts.reshape(1, LANES),
        partials,
        residual.reshape(square),
        weight.reshape(square),
        prior,
    )
    vmem = pl.BlockSpec(memory_space=pltpu.VMEM)
    updates, standard, norm = pl.pallas_call(
        functools.partial(kernel, shape),
        out_shape=(
            jax.ShapeDtypeStruct((PARAMS, LANES), F32),
            jax.ShapeDtypeStruct(square, F32),
            jax.ShapeDtypeStruct((1, LANES), F32),
        ),
        in_specs=[pl.BlockSpec(memory_space=pl.ANY)] * 8,
        out_specs=(vmem, vmem, vmem),
        scratch_shapes=[pltpu.VMEM(array.shape, array.dtype) for array in arrays]
        + [
            pltpu.VMEM((chips * 8, LANES), F32),
            pltpu.VMEM((chips * 8, LANES), F32),
            pltpu.VMEM((CORES, chips * 4, LANES), F32),
            pltpu.VMEM((CORES, LANES, chips * LANES // 2), BF16),
            pltpu.VMEM((CORES, LANES, GROUP // 2 * LANES), BF16),
            pltpu.VMEM((CORES, LANES, LANES), F32),
            pltpu.VMEM((CORES, 2, LANES, LANES), F32),
            pltpu.VMEM((CORES * 8, LANES), F32),
            pltpu.VMEM((CORES * PARAMS * 8, LANES), F32),
            pltpu.VMEM((CORES * PARAMS * 8, LANES), F32),
            pltpu.VMEM((CORES * 8, LANES), F32),
            pltpu.VMEM((chips, 1, LANES), F32),
            pltpu.VMEM((chips, 1, LANES), F32),
            pltpu.VMEM((3, 1, LANES), F32),
            pltpu.VMEM((chips, 1, LANES), F32),
            pltpu.VMEM((1, LANES), F32),
            pltpu.SemaphoreType.DMA((8,)),
            pltpu.SemaphoreType.DMA,
            pltpu.SemaphoreType.DMA((groups,)),
            pltpu.SemaphoreType.DMA((3,)),
            pltpu.SemaphoreType.DMA((3,)),
            pltpu.SemaphoreType.DMA((2,)),
            pltpu.SemaphoreType.DMA((2,)),
        ],
        compiler_params=pltpu.CompilerParams(collective_id=0, has_side_effects=True),
    )(*arrays)
    return updates, standard.reshape(-1), norm[0, 0]


def solution(mesh):
    shape = (mesh.shape["grp"], ROWS_Y, mesh.shape["dev"] // (ROWS_Y * CORES))
    rows = P(("grp", "dev"))
    columns = P(None, ("grp", "dev"))
    in_specs = (rows, rows, P(), rows, columns, rows, rows, columns)
    out_specs = (columns, rows, P())
    return jax.shard_map(
        functools.partial(body, shape), mesh=mesh, in_specs=in_specs, out_specs=out_specs, check_vma=False
    )
```

```python
import functools

import jax
import jax.numpy as jnp
from jax import lax
from jax.experimental import pallas as pl
from jax.experimental.pallas import tpu as pltpu
from jax.sharding import PartitionSpec as P

MESH = pl.DeviceIdType.MESH
F32 = jnp.float32
BF16 = jnp.bfloat16
LANES = 128
ROWS_Y = 4
CORES = 2
PARAMS = 5
FIELDS = 7
GROUP = 16
WIDE = GROUP // 2 * LANES
PACK = 16


def split_bf16(value):
    high = value.astype(BF16).astype(F32)
    rest = value - high
    middle = rest.astype(BF16).astype(F32)
    return high, middle, rest - middle


def column_of(row):
    square = (LANES, LANES)
    diagonal = lax.broadcasted_iota(jnp.int32, square, 0) == lax.broadcasted_iota(jnp.int32, square, 1)
    return jnp.sum(jnp.where(diagonal, jnp.broadcast_to(row, square), 0.0), axis=1, keepdims=True)


def solve_blocks(normal, moments):
    params = len(moments)
    factor = {}
    for column in range(params):
        running = normal[column][column]
        for earlier in range(column):
            running = running - factor[column, earlier] ** 2
        pivot_value = jnp.sqrt(running)
        factor[column, column] = pivot_value
        for target in range(column + 1, params):
            current = normal[target][column]
            for earlier in range(column):
                current = current - factor[target, earlier] * factor[column, earlier]
            factor[target, column] = current / pivot_value
    forward = []
    for target in range(params):
        current = moments[target]
        for earlier in range(target):
            current = current - factor[target, earlier] * forward[earlier]
        forward.append(current / factor[target, target])
    backward = [None] * params
    for target in reversed(range(params)):
        current = forward[target]
        for later in range(target + 1, params):
            current = current - factor[later, target] * backward[later]
        backward[target] = current / factor[target, target]
    return backward


def send_order(shape):
    size_x, size_y, size_z = shape
    far_x, far_y, far_z = (
        sorted(range(size), key=lambda step: (-min(step, size - step), step)) for size in (size_x, size_y, size_z)
    )
    return [(dx, dy, dz) for dy in far_y for dz in far_z for dx in far_x]


def kernel(
    shape,
    *refs,
):
    inputs, (updates_ref, standard_ref, norm_ref) = refs[0:8], refs[8:11]
    loaded = refs[11:19]
    (send_buf, recv_buf, halves, onehot, stats, total, table, facts, sums, other_sums) = refs[19:29]
    (update_rows, fresh_out, fresh_in, squares_mine, squares_other) = refs[29:34]
    (load_sem, send_sem, recv_sem, pair_send, pair_recv, back_send, back_recv) = refs[34:41]
    size_x, size_y, size_z = shape
    chips = size_x * size_y * size_z
    groups = chips // GROUP
    me_x = lax.axis_index("grp")
    me_dev = lax.axis_index("dev")
    core = me_dev % CORES
    me_y = (me_dev // CORES) % size_y
    me_z = me_dev // (CORES * size_y)
    me_chip = (me_x * size_z + me_z) * size_y + me_y


    xs = [(me_x + dx) % size_x for dx in range(size_x)]
    ys = [(me_y + dy) % size_y for dy in range(size_y)]
    zs = [(me_z + dz) % size_z for dz in range(size_z)]
    offsets = send_order(shape)

    def everywhere(forward, action):
        for slot, (dx, dy, dz) in enumerate(offsets[:-1]):
            if not forward:
                dx, dy, dz = (size_x - dx) % size_x, (size_y - dy) % size_y, (size_z - dz) % size_z
            action(slot, xs[dx], zs[dz] * size_y + ys[dy])

    partner = (me_x, me_dev + 1 - 2 * core)
    barrier = pltpu.get_barrier_semaphore()

    loads = [
        pltpu.make_async_copy(source, target, load_sem.at[index])
        for index, (source, target) in enumerate(zip(inputs, loaded, strict=True))
    ]
    for load in loads:
        load.start()
    for block in range(chips // 8):
        recv_buf[pl.ds(block * 64 + FIELDS, 8, stride=8), :] = jnp.zeros((8, LANES), F32)

    pl.semaphore_signal(barrier, inc=1, device_id=partner, device_id_type=MESH)
    everywhere(
        True,
        lambda slot, x, zy: pl.semaphore_signal(
            barrier, inc=1, device_id=(x, zy * CORES + core), device_id_type=MESH
        ),
    )

    source_ref, slot_ref, owner_ref, counts_ref, partials_ref, residual_ref, weight_ref, prior_ref = loaded
    for load in loads:
        load.wait()

    for block in range(chips // 8):
        rows = pl.ds(block * 8, 8)
        root = jnp.sqrt(weight_ref[rows, :])
        cell = (source_ref[rows, :] * LANES + slot_ref[rows, :]).astype(F32)
        send_buf[pl.ds(block * 64 + PARAMS, 8, stride=8), :] = residual_ref[rows, :] * root
        send_buf[pl.ds(block * 64 + PARAMS + 1, 8, stride=8), :] = cell
        for row in range(8):
            tile = block * 8 + row
            send_buf[tile * 8 : tile * 8 + PARAMS, :] = (
                partials_ref[:, tile * LANES : (tile + 1) * LANES] * root[row : row + 1, :]
            )
    facts[pl.ds(pl.multiple_of(core * 8, 8), 8), :] = jnp.concatenate(
        [prior_ref[...], counts_ref[...].astype(F32), jnp.zeros((2, LANES), F32)], axis=0
    )

    pl.semaphore_wait(barrier, chips)

    facts_copy = pltpu.make_async_remote_copy(
        src_ref=facts.at[pl.ds(pl.multiple_of(core * 8, 8), 8), :],
        dst_ref=facts.at[pl.ds(pl.multiple_of(core * 8, 8), 8), :],
        send_sem=pair_send.at[0],
        recv_sem=pair_recv.at[0],
        device_id=partner,
        device_id_type=MESH,
    )
    facts_copy.start()

    def send_tile(slot, x, zy):
        chip = x * (size_z * size_y) + zy
        pltpu.make_async_remote_copy(
            src_ref=send_buf.at[pl.ds(pl.multiple_of(chip * 8, 8), FIELDS), :],
            dst_ref=recv_buf.at[pl.ds(slot * 8, FIELDS), :],
            send_sem=send_sem,
            recv_sem=recv_sem.at[slot // GROUP],
            device_id=(x, zy * CORES + core),
            device_id_type=MESH,
        ).start()

    everywhere(True, send_tile)
    recv_buf[(chips - 1) * 8 : chips * 8 - 1, :] = send_buf[pl.ds(pl.multiple_of(me_chip * 8, 8), 8), :][0:FIELDS, :]

    sublane = lax.broadcasted_iota(jnp.int32, (LANES, LANES), 0)
    lane = lax.broadcasted_iota(jnp.int32, (1, LANES), 1)
    for side in range(CORES):
        base = (me_chip * CORES + side) * LANES

        def look(step, found):
            rows = owner_ref[pl.ds(pl.multiple_of(step * 8, 8), 8), :] - base
            for row in range(8):
                here = lane + (step * 8 + row) * LANES
                found = jnp.where(rows[row : row + 1, :] == sublane, here, found)
            return found

        found = lax.fori_loop(0, owner_ref.shape[0] // 8, look, jnp.zeros((LANES, LANES), jnp.int32))
        first = jnp.sum(found.astype(F32), axis=1, keepdims=True)
        table[side, 0] = jnp.broadcast_to(first, (LANES, LANES)).astype(jnp.int32).astype(jnp.int16)

    facts_copy.wait()
    for side in range(CORES):
        count = column_of(facts[side * 8 + PARAMS : side * 8 + PARAMS + 1, :])
        table[side, 1] = jnp.broadcast_to(count, (LANES, LANES)).astype(jnp.int32).astype(jnp.int16)

    def wait_rows(source, target, count, send, recv, to):
        return pltpu.make_async_remote_copy(
            src_ref=source.at[pl.ds(0, count)],
            dst_ref=target.at[pl.ds(0, count)],
            send_sem=send,
            recv_sem=recv,
            device_id=to,
            device_id_type=MESH,
        )

    low = lax.broadcasted_iota(jnp.int32, (8, LANES), 1) < LANES // 2
    total[...] = jnp.zeros_like(total)

    def gather_group(q):
        sides = ([], [])
        for v in range(GROUP // 2):
            start = (q * GROUP + v * 2) * 8
            even = recv_buf[start : start + 8, :]
            odd = recv_buf[start + 8 : start + 16, :]
            sides[0].append(jnp.where(low, even, pltpu.roll(odd, LANES // 2, 1)))
            sides[1].append(jnp.where(low, pltpu.roll(even, LANES // 2, 1), odd))
        for side in range(CORES):
            sources, slots = [], []
            for v, rows in enumerate(sides[side]):
                place = (q * (GROUP // 2) + v) * 8
                halves[side, place : place + 8, :] = rows
                cell = jnp.broadcast_to(rows[FIELDS - 1 : FIELDS, :], (PACK, LANES)).astype(jnp.int32)
                sources.append((cell // LANES).astype(jnp.int16))
                slots.append((cell % LANES).astype(jnp.int16))
                terms = jnp.concatenate([rows[i : i + 1, :] * rows for i in range(PARAMS)], axis=0)
                parts = jnp.concatenate([*split_bf16(terms), jnp.zeros((8, LANES), F32)], axis=0)
                stats[side, :, q * WIDE + v * LANES : q * WIDE + (v + 1) * LANES] = parts.astype(BF16)
            for part in range(LANES // PACK):
                picked = slice(part * PACK, (part + 1) * PACK)
                source, count = table[side, 0, picked, :], table[side, 1, picked, :]
                for v in range(GROUP // 2):
                    inside = (sources[v] == source) & (slots[v] < count)
                    onehot[side, picked, q * WIDE + v * LANES : q * WIDE + (v + 1) * LANES] = jnp.where(
                        inside, jnp.ones((PACK, LANES), BF16), jnp.zeros((PACK, LANES), BF16)
                    )

    def sum_group(q):
        for side in range(CORES):
            where = slice(q * WIDE, (q + 1) * WIDE)
            total[side] += lax.dot_general(
                stats[side, :, where],
                onehot[side, :, where],
                (((1,), (1,)), ((), ())),
                preferred_element_type=F32,
            )

    order = list(range(groups))
    for at, q in enumerate(order):
        count = GROUP - 1 if q == groups - 1 else GROUP
        wait_rows(send_buf, recv_buf, count * FIELDS, send_sem, recv_sem.at[q], partner).wait_recv()
        gather_group(q)
        if at > 0:
            sum_group(order[at - 1])
    sum_group(order[-1])

    span = PARAMS * 8
    for side in range(CORES):
        sums[side * span : (side + 1) * span, :] = (
            total[side, 0:span, :] + total[side, span : 2 * span, :] + total[side, 2 * span : 3 * span, :]
        )
    sums_copy = pltpu.make_async_remote_copy(
        src_ref=sums,
        dst_ref=other_sums,
        send_sem=pair_send.at[1],
        recv_sem=pair_recv.at[1],
        device_id=partner,
        device_id_type=MESH,
    )
    sums_copy.start()
    sums_copy.wait_recv()

    def summed(row):
        rows = pl.ds(row, CORES, stride=span)
        return sums[rows, :] + other_sums[rows, :]

    normal = [[None] * PARAMS for _ in range(PARAMS)]
    for i in range(PARAMS):
        for j in range(i, PARAMS):
            entry = summed(i * 8 + j)
            if i == j:
                entry = entry + facts[pl.ds(i, CORES, stride=8), :]
            normal[i][j] = entry
            normal[j][i] = entry
    moments = [summed(i * 8 + PARAMS) for i in range(PARAMS)]
    updates = solve_blocks(normal, moments)
    for i in range(PARAMS):
        update_rows[pl.ds(i, CORES, stride=8), :] = updates[i]
    update_rows[pl.ds(PARAMS, CORES, stride=8), :] = jnp.full((CORES, LANES), -1.0, F32)
    for row in (PARAMS + 1, PARAMS + 2):
        update_rows[pl.ds(row, CORES, stride=8), :] = jnp.zeros((CORES, LANES), F32)
    updates_ref[...] = update_rows[pl.ds(pl.multiple_of(core * 8, 8), 8), :][0:PARAMS, :]

    spread = []
    for side in range(CORES):
        parts = split_bf16(update_rows[side * 8 : side * 8 + 8, :])
        spread.append(jnp.concatenate([*parts, jnp.zeros((8, LANES), F32)], axis=0).astype(BF16))

    squares = jnp.zeros((1, LANES), F32)
    for q in range(groups):
        fitted = []
        for side in range(CORES):
            got = lax.dot_general(
                spread[side],
                onehot[side, :, q * WIDE : (q + 1) * WIDE],
                (((1,), (0,)), ((), ())),
                preferred_element_type=F32,
            )
            fitted.append(got[0:8, :] + got[8:16, :] + got[16:24, :])
        for v in range(GROUP // 2):
            fresh = []
            for side in range(CORES):
                rows = halves[side, (q * GROUP // 2 + v) * 8 : (q * GROUP // 2 + v + 1) * 8, :]
                term = rows * fitted[side][:, v * LANES : (v + 1) * LANES]
                line = -jnp.sum(term, axis=0, keepdims=True)
                squares = squares + line * line
                fresh.append(line)
            left, right = fresh
            at = q * GROUP + v * 2
            fresh_out[at, 0:1] = jnp.where(low[0:1], left, pltpu.roll(right, LANES // 2, 1))
            fresh_out[at + 1, 0:1] = jnp.where(low[0:1], pltpu.roll(left, LANES // 2, 1), right)
    count_row = counts_ref[...].astype(F32)
    squares = squares + pltpu.roll(squares, LANES // 2, 1)
    count_row = count_row + pltpu.roll(count_row, LANES // 2, 1)
    square_row = jnp.where(low[0:1], squares, count_row)
    for slot in range(chips):
        fresh_out[slot, 1:2] = square_row

    def send_fresh(slot, x, zy):
        pltpu.make_async_remote_copy(
            src_ref=fresh_out.at[slot],
            dst_ref=fresh_in.at[me_chip],
            send_sem=back_send,
            recv_sem=back_recv,
            device_id=(x, zy * CORES + core),
            device_id_type=MESH,
        ).start()

    everywhere(False, send_fresh)
    fresh_in[me_chip] = fresh_out[chips - 1]
    wait_rows(fresh_in, fresh_in, chips - 1, back_send, back_recv, partner).wait_recv()
    squares_mine[...] = jnp.sum(fresh_in[:, 1, :], axis=0, keepdims=True)
    square_copy = pltpu.make_async_remote_copy(
        src_ref=squares_mine,
        dst_ref=squares_other,
        send_sem=pair_send.at[2],
        recv_sem=pair_recv.at[2],
        device_id=partner,
        device_id_type=MESH,
    )
    square_copy.start()
    fresh = fresh_in[:, 0, :]
    square_copy.wait_recv()
    whole = squares_mine[...] + squares_other[...]
    square_sum = jnp.sum(jnp.where(low[0:1], whole, 0.0), axis=1, keepdims=True)
    count_sum = jnp.sum(jnp.where(low[0:1], 0.0, whole), axis=1, keepdims=True)
    norm = jnp.sqrt(square_sum / count_sum + 1e-6)
    norm_ref[...] = jnp.broadcast_to(norm, (1, LANES))
    standard_ref[...] = fresh / norm

    wait_rows(send_buf, recv_buf, (chips - 1) * FIELDS, send_sem, send_sem, partner).wait_send()
    sums_copy.wait_send()
    square_copy.wait_send()
    wait_rows(fresh_in, fresh_in, chips - 1, back_send, back_recv, partner).wait_send()


def finish(*refs):
    copies = [
        pltpu.make_async_copy(source, target, refs[6].at[index])
        for index, (source, target) in enumerate(zip(refs[0:3], refs[3:6], strict=True))
    ]
    for copy in copies:
        copy.start()
    for copy in copies:
        copy.wait()


def body(shape, source_id, slot, owner, counts, partials, residual, weight, prior):
    size_x, size_y, size_z = shape
    chips = size_x * size_y * size_z
    groups = chips // GROUP
    square = (chips, LANES)
    arrays = (
        source_id.reshape(square),
        slot.reshape(square),
        owner.reshape(-1, LANES),
        counts.reshape(1, LANES),
        partials,
        residual.reshape(square),
        weight.reshape(square),
        prior,
    )
    vmem = pl.BlockSpec(memory_space=pltpu.VMEM)
    results = (
        jax.ShapeDtypeStruct((PARAMS, LANES), F32),
        jax.ShapeDtypeStruct(square, F32),
        jax.ShapeDtypeStruct((1, LANES), F32),
    )
    exchanged = pl.pallas_call(
        functools.partial(kernel, shape),
        out_shape=tuple(pltpu.VMEM(result.shape, result.dtype) for result in results),
        in_specs=[pl.BlockSpec(memory_space=pl.ANY)] * 8,
        out_specs=(vmem, vmem, vmem),
        scratch_shapes=[pltpu.VMEM(array.shape, array.dtype) for array in arrays]
        + [
            pltpu.VMEM((chips * 8, LANES), F32),
            pltpu.VMEM((chips * 8, LANES), F32),
            pltpu.VMEM((CORES, chips * 4, LANES), F32),
            pltpu.VMEM((CORES, LANES, chips * LANES // 2), BF16),
            pltpu.VMEM((CORES, LANES, chips * LANES // 2), BF16),
            pltpu.VMEM((CORES, LANES, LANES), F32),
            pltpu.VMEM((CORES, 2, LANES, LANES), jnp.int16),
            pltpu.VMEM((CORES * 8, LANES), F32),
            pltpu.VMEM((CORES * PARAMS * 8, LANES), F32),
            pltpu.VMEM((CORES * PARAMS * 8, LANES), F32),
            pltpu.VMEM((CORES * 8, LANES), F32),
            pltpu.VMEM((chips, 2, LANES), F32),
            pltpu.VMEM((chips, 2, LANES), F32),
            pltpu.VMEM((1, LANES), F32),
            pltpu.VMEM((1, LANES), F32),
            pltpu.SemaphoreType.DMA((8,)),
            pltpu.SemaphoreType.DMA,
            pltpu.SemaphoreType.DMA((groups,)),
            pltpu.SemaphoreType.DMA((3,)),
            pltpu.SemaphoreType.DMA((3,)),
            pltpu.SemaphoreType.DMA,
            pltpu.SemaphoreType.DMA,
        ],
        compiler_params=pltpu.CompilerParams(collective_id=0, has_side_effects=True),
    )(*arrays)
    place = pl.BlockSpec(memory_space=pl.ANY)
    updates, standard, norm = pl.pallas_call(
        finish,
        out_shape=results,
        in_specs=[place] * 3,
        out_specs=(place, place, place),
        scratch_shapes=[pltpu.SemaphoreType.DMA((3,))],
    )(*(pltpu.with_memory_space_constraint(value, pltpu.VMEM) for value in exchanged))
    return updates, standard.reshape(-1), norm[0, 0]


def solution(mesh):
    shape = (mesh.shape["grp"], ROWS_Y, mesh.shape["dev"] // (ROWS_Y * CORES))
    rows = P(("grp", "dev"))
    columns = P(None, ("grp", "dev"))
    in_specs = (rows, rows, P(), rows, columns, rows, rows, columns)
    out_specs = (columns, rows, P())
    return jax.shard_map(
        functools.partial(body, shape), mesh=mesh, in_specs=in_specs, out_specs=out_specs, check_vma=False
    )
```

```python
import functools

import jax
import jax.numpy as jnp
from jax import lax
from jax.experimental import pallas as pl
from jax.experimental.pallas import tpu as pltpu
from jax.sharding import PartitionSpec as P

MESH = pl.DeviceIdType.MESH
F32 = jnp.float32
BF16 = jnp.bfloat16
LANES = 128
ROWS_Y = 4
CORES = 2
PARAMS = 5
FIELDS = 7
GROUP = 16
WIDE = GROUP // 2 * LANES
PACK = 16


def split_bf16(value):
    high = value.astype(BF16).astype(F32)
    rest = value - high
    middle = rest.astype(BF16).astype(F32)
    return high, middle, rest - middle


def column_of(row):
    square = (LANES, LANES)
    diagonal = lax.broadcasted_iota(jnp.int32, square, 0) == lax.broadcasted_iota(jnp.int32, square, 1)
    return jnp.sum(jnp.where(diagonal, jnp.broadcast_to(row, square), 0.0), axis=1, keepdims=True)


def solve_blocks(normal, moments):
    params = len(moments)
    factor = {}
    for column in range(params):
        running = normal[column][column]
        for earlier in range(column):
            running = running - factor[column, earlier] ** 2
        pivot_value = jnp.sqrt(running)
        factor[column, column] = pivot_value
        for target in range(column + 1, params):
            current = normal[target][column]
            for earlier in range(column):
                current = current - factor[target, earlier] * factor[column, earlier]
            factor[target, column] = current / pivot_value
    forward = []
    for target in range(params):
        current = moments[target]
        for earlier in range(target):
            current = current - factor[target, earlier] * forward[earlier]
        forward.append(current / factor[target, target])
    backward = [None] * params
    for target in reversed(range(params)):
        current = forward[target]
        for later in range(target + 1, params):
            current = current - factor[later, target] * backward[later]
        backward[target] = current / factor[target, target]
    return backward


def hops(offset, shape):
    return sum(min(step, size - step) for step, size in zip(offset, shape, strict=True))


def send_order(shape):
    size_x, size_y, size_z = shape
    reach = size_z // 4
    every = [(x, y, z) for y in range(size_y) for z in range(size_z) for x in range(size_x)]
    every.sort(key=lambda offset: -hops(offset, shape))
    near = [offset for offset in every[:-1] if min(offset[2], size_z - offset[2]) <= reach]
    far = [offset for offset in every[:-1] if offset not in near]
    return near, far, [(0, 0, reach), (0, 0, size_z - reach)]


def kernel(
    shape,
    *refs,
):
    inputs, (updates_ref, standard_ref, norm_ref) = refs[0:8], refs[8:11]
    loaded = refs[11:19]
    (send_buf, recv_buf, halves, onehot, stats, total, table, facts, sums, other_sums) = refs[19:29]
    (update_rows, fresh_out, fresh_in, squares_mine, squares_other) = refs[29:34]
    (load_sem, send_sem, recv_sem, pair_send, pair_recv, back_send, back_recv, vouched) = refs[34:42]
    size_x, size_y, size_z = shape
    chips = size_x * size_y * size_z
    groups = chips // GROUP
    me_x = lax.axis_index("grp")
    me_dev = lax.axis_index("dev")
    core = me_dev % CORES
    me_y = (me_dev // CORES) % size_y
    me_z = me_dev // (CORES * size_y)
    me_chip = (me_x * size_z + me_z) * size_y + me_y


    xs = [(me_x + dx) % size_x for dx in range(size_x)]
    ys = [(me_y + dy) % size_y for dy in range(size_y)]
    zs = [(me_z + dz) % size_z for dz in range(size_z)]
    near, far, vouchers = send_order(shape)
    offsets = near + far
    nearby, beyond = range(len(near)), range(len(near), len(offsets))

    def ahead(offset):
        dx, dy, dz = offset
        return xs[dx], zs[dz] * size_y + ys[dy]

    def behind(offset):
        dx, dy, dz = offset
        return ahead(((size_x - dx) % size_x, (size_y - dy) % size_y, (size_z - dz) % size_z))

    partner = (me_x, me_dev + 1 - 2 * core)
    barrier = pltpu.get_barrier_semaphore()

    loads = [
        pltpu.make_async_copy(source, target, load_sem.at[index])
        for index, (source, target) in enumerate(zip(inputs, loaded, strict=True))
    ]
    for load in loads:
        load.start()
    for block in range(chips // 8):
        recv_buf[pl.ds(block * 64 + FIELDS, 8, stride=8), :] = jnp.zeros((8, LANES), F32)

    pl.semaphore_signal(barrier, inc=1, device_id=partner, device_id_type=MESH)
    for offset in near:
        x, zy = ahead(offset)
        pl.semaphore_signal(barrier, inc=1, device_id=(x, zy * CORES + core), device_id_type=MESH)

    source_ref, slot_ref, owner_ref, counts_ref, partials_ref, residual_ref, weight_ref, prior_ref = loaded
    for load in loads:
        load.wait()

    for block in range(chips // 8):
        rows = pl.ds(block * 8, 8)
        root = jnp.sqrt(weight_ref[rows, :])
        cell = (source_ref[rows, :] * LANES + slot_ref[rows, :]).astype(F32)
        send_buf[pl.ds(block * 64 + PARAMS, 8, stride=8), :] = residual_ref[rows, :] * root
        send_buf[pl.ds(block * 64 + PARAMS + 1, 8, stride=8), :] = cell
        for row in range(8):
            tile = block * 8 + row
            send_buf[tile * 8 : tile * 8 + PARAMS, :] = (
                partials_ref[:, tile * LANES : (tile + 1) * LANES] * root[row : row + 1, :]
            )
    facts[pl.ds(pl.multiple_of(core * 8, 8), 8), :] = jnp.concatenate(
        [prior_ref[...], counts_ref[...].astype(F32), jnp.zeros((2, LANES), F32)], axis=0
    )

    pl.semaphore_wait(barrier, len(near) + 1)
    for offset in vouchers:
        x, zy = behind(offset)
        pl.semaphore_signal(vouched, inc=1, device_id=(x, zy * CORES + core), device_id_type=MESH)

    facts_copy = pltpu.make_async_remote_copy(
        src_ref=facts.at[pl.ds(pl.multiple_of(core * 8, 8), 8), :],
        dst_ref=facts.at[pl.ds(pl.multiple_of(core * 8, 8), 8), :],
        send_sem=pair_send.at[0],
        recv_sem=pair_recv.at[0],
        device_id=partner,
        device_id_type=MESH,
    )
    facts_copy.start()

    def send_tile(slot):
        x, zy = ahead(offsets[slot])
        chip = x * (size_z * size_y) + zy
        pltpu.make_async_remote_copy(
            src_ref=send_buf.at[pl.ds(pl.multiple_of(chip * 8, 8), FIELDS), :],
            dst_ref=recv_buf.at[pl.ds(slot * 8, FIELDS), :],
            send_sem=send_sem,
            recv_sem=recv_sem.at[slot // GROUP],
            device_id=(x, zy * CORES + core),
            device_id_type=MESH,
        ).start()

    for slot in nearby:
        send_tile(slot)
    pl.semaphore_wait(vouched, len(vouchers))
    for slot in beyond:
        send_tile(slot)
    recv_buf[(chips - 1) * 8 : chips * 8 - 1, :] = send_buf[pl.ds(pl.multiple_of(me_chip * 8, 8), 8), :][0:FIELDS, :]

    sublane = lax.broadcasted_iota(jnp.int32, (LANES, LANES), 0)
    lane = lax.broadcasted_iota(jnp.int32, (1, LANES), 1)
    for side in range(CORES):
        base = (me_chip * CORES + side) * LANES

        def look(step, found):
            rows = owner_ref[pl.ds(pl.multiple_of(step * 8, 8), 8), :] - base
            for row in range(8):
                here = lane + (step * 8 + row) * LANES
                found = jnp.where(rows[row : row + 1, :] == sublane, here, found)
            return found

        found = lax.fori_loop(0, owner_ref.shape[0] // 8, look, jnp.zeros((LANES, LANES), jnp.int32))
        first = jnp.sum(found.astype(F32), axis=1, keepdims=True)
        table[side, 0] = jnp.broadcast_to(first, (LANES, LANES)).astype(jnp.int32).astype(jnp.int16)

    facts_copy.wait()
    for side in range(CORES):
        count = column_of(facts[side * 8 + PARAMS : side * 8 + PARAMS + 1, :])
        table[side, 1] = jnp.broadcast_to(count, (LANES, LANES)).astype(jnp.int32).astype(jnp.int16)

    def wait_rows(source, target, count, send, recv, to):
        return pltpu.make_async_remote_copy(
            src_ref=source.at[pl.ds(0, count)],
            dst_ref=target.at[pl.ds(0, count)],
            send_sem=send,
            recv_sem=recv,
            device_id=to,
            device_id_type=MESH,
        )

    low = lax.broadcasted_iota(jnp.int32, (8, LANES), 1) < LANES // 2
    total[...] = jnp.zeros_like(total)

    def gather_group(q):
        sides = ([], [])
        for v in range(GROUP // 2):
            start = (q * GROUP + v * 2) * 8
            even = recv_buf[start : start + 8, :]
            odd = recv_buf[start + 8 : start + 16, :]
            sides[0].append(jnp.where(low, even, pltpu.roll(odd, LANES // 2, 1)))
            sides[1].append(jnp.where(low, pltpu.roll(even, LANES // 2, 1), odd))
        for side in range(CORES):
            sources, slots = [], []
            for v, rows in enumerate(sides[side]):
                place = (q * (GROUP // 2) + v) * 8
                halves[side, place : place + 8, :] = rows
                cell = jnp.broadcast_to(rows[FIELDS - 1 : FIELDS, :], (PACK, LANES)).astype(jnp.int32)
                sources.append((cell // LANES).astype(jnp.int16))
                slots.append((cell % LANES).astype(jnp.int16))
                terms = jnp.concatenate([rows[i : i + 1, :] * rows for i in range(PARAMS)], axis=0)
                parts = jnp.concatenate([*split_bf16(terms), jnp.zeros((8, LANES), F32)], axis=0)
                stats[side, :, q * WIDE + v * LANES : q * WIDE + (v + 1) * LANES] = parts.astype(BF16)
            for part in range(LANES // PACK):
                picked = slice(part * PACK, (part + 1) * PACK)
                source, count = table[side, 0, picked, :], table[side, 1, picked, :]
                for v in range(GROUP // 2):
                    inside = (sources[v] == source) & (slots[v] < count)
                    onehot[side, picked, q * WIDE + v * LANES : q * WIDE + (v + 1) * LANES] = jnp.where(
                        inside, jnp.ones((PACK, LANES), BF16), jnp.zeros((PACK, LANES), BF16)
                    )

    def sum_group(q):
        for side in range(CORES):
            where = slice(q * WIDE, (q + 1) * WIDE)
            total[side] += lax.dot_general(
                stats[side, :, where],
                onehot[side, :, where],
                (((1,), (1,)), ((), ())),
                preferred_element_type=F32,
            )

    order = list(range(groups))
    for at, q in enumerate(order):
        count = GROUP - 1 if q == groups - 1 else GROUP
        wait_rows(send_buf, recv_buf, count * FIELDS, send_sem, recv_sem.at[q], partner).wait_recv()
        gather_group(q)
        if at > 0:
            sum_group(order[at - 1])
    sum_group(order[-1])

    span = PARAMS * 8
    for side in range(CORES):
        sums[side * span : (side + 1) * span, :] = (
            total[side, 0:span, :] + total[side, span : 2 * span, :] + total[side, 2 * span : 3 * span, :]
        )
    sums_copy = pltpu.make_async_remote_copy(
        src_ref=sums,
        dst_ref=other_sums,
        send_sem=pair_send.at[1],
        recv_sem=pair_recv.at[1],
        device_id=partner,
        device_id_type=MESH,
    )
    sums_copy.start()
    sums_copy.wait_recv()

    def summed(row):
        rows = pl.ds(row, CORES, stride=span)
        return sums[rows, :] + other_sums[rows, :]

    normal = [[None] * PARAMS for _ in range(PARAMS)]
    for i in range(PARAMS):
        for j in range(i, PARAMS):
            entry = summed(i * 8 + j)
            if i == j:
                entry = entry + facts[pl.ds(i, CORES, stride=8), :]
            normal[i][j] = entry
            normal[j][i] = entry
    moments = [summed(i * 8 + PARAMS) for i in range(PARAMS)]
    updates = solve_blocks(normal, moments)
    for i in range(PARAMS):
        update_rows[pl.ds(i, CORES, stride=8), :] = updates[i]
    update_rows[pl.ds(PARAMS, CORES, stride=8), :] = jnp.full((CORES, LANES), -1.0, F32)
    for row in (PARAMS + 1, PARAMS + 2):
        update_rows[pl.ds(row, CORES, stride=8), :] = jnp.zeros((CORES, LANES), F32)
    updates_ref[...] = update_rows[pl.ds(pl.multiple_of(core * 8, 8), 8), :][0:PARAMS, :]

    spread = []
    for side in range(CORES):
        parts = split_bf16(update_rows[side * 8 : side * 8 + 8, :])
        spread.append(jnp.concatenate([*parts, jnp.zeros((8, LANES), F32)], axis=0).astype(BF16))

    squares = jnp.zeros((1, LANES), F32)
    for q in range(groups):
        fitted = []
        for side in range(CORES):
            got = lax.dot_general(
                spread[side],
                onehot[side, :, q * WIDE : (q + 1) * WIDE],
                (((1,), (0,)), ((), ())),
                preferred_element_type=F32,
            )
            fitted.append(got[0:8, :] + got[8:16, :] + got[16:24, :])
        for v in range(GROUP // 2):
            fresh = []
            for side in range(CORES):
                rows = halves[side, (q * GROUP // 2 + v) * 8 : (q * GROUP // 2 + v + 1) * 8, :]
                term = rows * fitted[side][:, v * LANES : (v + 1) * LANES]
                line = -jnp.sum(term, axis=0, keepdims=True)
                squares = squares + line * line
                fresh.append(line)
            left, right = fresh
            at = q * GROUP + v * 2
            fresh_out[at, 0:1] = jnp.where(low[0:1], left, pltpu.roll(right, LANES // 2, 1))
            fresh_out[at + 1, 0:1] = jnp.where(low[0:1], pltpu.roll(left, LANES // 2, 1), right)
    count_row = counts_ref[...].astype(F32)
    squares = squares + pltpu.roll(squares, LANES // 2, 1)
    count_row = count_row + pltpu.roll(count_row, LANES // 2, 1)
    square_row = jnp.where(low[0:1], squares, count_row)
    for slot in range(chips):
        fresh_out[slot, 1:2] = square_row

    def send_fresh(slot):
        x, zy = behind(offsets[slot])
        pltpu.make_async_remote_copy(
            src_ref=fresh_out.at[slot],
            dst_ref=fresh_in.at[me_chip],
            send_sem=back_send,
            recv_sem=back_recv,
            device_id=(x, zy * CORES + core),
            device_id_type=MESH,
        ).start()

    for slot in sorted(range(chips - 1), key=lambda slot: -hops(offsets[slot], shape)):
        send_fresh(slot)
    fresh_in[me_chip] = fresh_out[chips - 1]
    wait_rows(fresh_in, fresh_in, chips - 1, back_send, back_recv, partner).wait_recv()
    squares_mine[...] = jnp.sum(fresh_in[:, 1, :], axis=0, keepdims=True)
    square_copy = pltpu.make_async_remote_copy(
        src_ref=squares_mine,
        dst_ref=squares_other,
        send_sem=pair_send.at[2],
        recv_sem=pair_recv.at[2],
        device_id=partner,
        device_id_type=MESH,
    )
    square_copy.start()
    fresh = fresh_in[:, 0, :]
    square_copy.wait_recv()
    whole = squares_mine[...] + squares_other[...]
    square_sum = jnp.sum(jnp.where(low[0:1], whole, 0.0), axis=1, keepdims=True)
    count_sum = jnp.sum(jnp.where(low[0:1], 0.0, whole), axis=1, keepdims=True)
    norm = jnp.sqrt(square_sum / count_sum + 1e-6)
    norm_ref[...] = jnp.broadcast_to(norm, (1, LANES))
    standard_ref[...] = fresh / norm

    wait_rows(send_buf, recv_buf, (chips - 1) * FIELDS, send_sem, send_sem, partner).wait_send()
    sums_copy.wait_send()
    square_copy.wait_send()
    wait_rows(fresh_in, fresh_in, chips - 1, back_send, back_recv, partner).wait_send()


def finish(*refs):
    copies = [
        pltpu.make_async_copy(source, target, refs[6].at[index])
        for index, (source, target) in enumerate(zip(refs[0:3], refs[3:6], strict=True))
    ]
    for copy in copies:
        copy.start()
    for copy in copies:
        copy.wait()


def body(shape, source_id, slot, owner, counts, partials, residual, weight, prior):
    size_x, size_y, size_z = shape
    chips = size_x * size_y * size_z
    groups = chips // GROUP
    square = (chips, LANES)
    arrays = (
        source_id.reshape(square),
        slot.reshape(square),
        owner.reshape(-1, LANES),
        counts.reshape(1, LANES),
        partials,
        residual.reshape(square),
        weight.reshape(square),
        prior,
    )
    vmem = pl.BlockSpec(memory_space=pltpu.VMEM)
    results = (
        jax.ShapeDtypeStruct((PARAMS, LANES), F32),
        jax.ShapeDtypeStruct(square, F32),
        jax.ShapeDtypeStruct((1, LANES), F32),
    )
    exchanged = pl.pallas_call(
        functools.partial(kernel, shape),
        out_shape=tuple(pltpu.VMEM(result.shape, result.dtype) for result in results),
        in_specs=[pl.BlockSpec(memory_space=pl.ANY)] * 8,
        out_specs=(vmem, vmem, vmem),
        scratch_shapes=[pltpu.VMEM(array.shape, array.dtype) for array in arrays]
        + [
            pltpu.VMEM((chips * 8, LANES), F32),
            pltpu.VMEM((chips * 8, LANES), F32),
            pltpu.VMEM((CORES, chips * 4, LANES), F32),
            pltpu.VMEM((CORES, LANES, chips * LANES // 2), BF16),
            pltpu.VMEM((CORES, LANES, chips * LANES // 2), BF16),
            pltpu.VMEM((CORES, LANES, LANES), F32),
            pltpu.VMEM((CORES, 2, LANES, LANES), jnp.int16),
            pltpu.VMEM((CORES * 8, LANES), F32),
            pltpu.VMEM((CORES * PARAMS * 8, LANES), F32),
            pltpu.VMEM((CORES * PARAMS * 8, LANES), F32),
            pltpu.VMEM((CORES * 8, LANES), F32),
            pltpu.VMEM((chips, 2, LANES), F32),
            pltpu.VMEM((chips, 2, LANES), F32),
            pltpu.VMEM((1, LANES), F32),
            pltpu.VMEM((1, LANES), F32),
            pltpu.SemaphoreType.DMA((8,)),
            pltpu.SemaphoreType.DMA,
            pltpu.SemaphoreType.DMA((groups,)),
            pltpu.SemaphoreType.DMA((3,)),
            pltpu.SemaphoreType.DMA((3,)),
            pltpu.SemaphoreType.DMA,
            pltpu.SemaphoreType.DMA,
            pltpu.SemaphoreType.REGULAR,
        ],
        compiler_params=pltpu.CompilerParams(collective_id=0, has_side_effects=True),
    )(*arrays)
    place = pl.BlockSpec(memory_space=pl.ANY)
    updates, standard, norm = pl.pallas_call(
        finish,
        out_shape=results,
        in_specs=[place] * 3,
        out_specs=(place, place, place),
        scratch_shapes=[pltpu.SemaphoreType.DMA((3,))],
    )(*(pltpu.with_memory_space_constraint(value, pltpu.VMEM) for value in exchanged))
    return updates, standard.reshape(-1), norm[0, 0]


def solution(mesh):
    shape = (mesh.shape["grp"], ROWS_Y, mesh.shape["dev"] // (ROWS_Y * CORES))
    rows = P(("grp", "dev"))
    columns = P(None, ("grp", "dev"))
    in_specs = (rows, rows, P(), rows, columns, rows, rows, columns)
    out_specs = (columns, rows, P())
    return jax.shard_map(
        functools.partial(body, shape), mesh=mesh, in_specs=in_specs, out_specs=out_specs, check_vma=False
    )
```

```python
import functools

import jax
import jax.numpy as jnp
from jax import lax
from jax.experimental import pallas as pl
from jax.experimental.pallas import tpu as pltpu
from jax.sharding import PartitionSpec as P

MESH = pl.DeviceIdType.MESH
F32 = jnp.float32
BF16 = jnp.bfloat16
F8 = jnp.float8_e4m3fn
LANES = 128
ROWS_Y = 4
CORES = 2
PARAMS = 5
FIELDS = 7
GROUP = 16
WIDE = GROUP // 2 * LANES
PACK = 16


def split_bf16(value):
    high = value.astype(BF16).astype(F32)
    rest = value - high
    middle = rest.astype(BF16).astype(F32)
    return high, middle, rest - middle


def column_of(row):
    square = (LANES, LANES)
    diagonal = lax.broadcasted_iota(jnp.int32, square, 0) == lax.broadcasted_iota(jnp.int32, square, 1)
    return jnp.sum(jnp.where(diagonal, jnp.broadcast_to(row, square), 0.0), axis=1, keepdims=True)


def solve_blocks(normal, moments):
    params = len(moments)
    factor = {}
    for column in range(params):
        running = normal[column][column]
        for earlier in range(column):
            running = running - factor[column, earlier] ** 2
        pivot_value = jnp.sqrt(running)
        factor[column, column] = pivot_value
        for target in range(column + 1, params):
            current = normal[target][column]
            for earlier in range(column):
                current = current - factor[target, earlier] * factor[column, earlier]
            factor[target, column] = current / pivot_value
    forward = []
    for target in range(params):
        current = moments[target]
        for earlier in range(target):
            current = current - factor[target, earlier] * forward[earlier]
        forward.append(current / factor[target, target])
    backward = [None] * params
    for target in reversed(range(params)):
        current = forward[target]
        for later in range(target + 1, params):
            current = current - factor[later, target] * backward[later]
        backward[target] = current / factor[target, target]
    return backward


def hops(offset, shape):
    return sum(min(step, size - step) for step, size in zip(offset, shape, strict=True))


def send_order(shape):
    size_x, size_y, size_z = shape
    reach = size_z // 4
    every = [(x, y, z) for y in range(size_y) for z in range(size_z) for x in range(size_x)]
    every.sort(key=lambda offset: -hops(offset, shape))
    near = [offset for offset in every[:-1] if min(offset[2], size_z - offset[2]) <= reach]
    far = [offset for offset in every[:-1] if offset not in near]
    return near, far, [(0, 0, reach), (0, 0, size_z - reach)]


def kernel(
    shape,
    *refs,
):
    inputs, (updates_ref, standard_ref, norm_ref) = refs[0:8], refs[8:11]
    loaded = refs[11:19]
    (send_buf, recv_buf, halves, onehot, total, table, facts, sums, other_sums) = refs[19:28]
    (update_rows, fresh_out, fresh_in, squares_mine, squares_other) = refs[28:33]
    (load_sem, send_sem, recv_sem, pair_send, pair_recv, back_send, back_recv, vouched) = refs[33:41]
    size_x, size_y, size_z = shape
    chips = size_x * size_y * size_z
    groups = chips // GROUP
    me_x = lax.axis_index("grp")
    me_dev = lax.axis_index("dev")
    core = me_dev % CORES
    me_y = (me_dev // CORES) % size_y
    me_z = me_dev // (CORES * size_y)
    me_chip = (me_x * size_z + me_z) * size_y + me_y


    xs = [(me_x + dx) % size_x for dx in range(size_x)]
    ys = [(me_y + dy) % size_y for dy in range(size_y)]
    zs = [(me_z + dz) % size_z for dz in range(size_z)]
    near, far, vouchers = send_order(shape)
    offsets = near + far
    nearby, beyond = range(len(near)), range(len(near), len(offsets))

    def ahead(offset):
        dx, dy, dz = offset
        return xs[dx], zs[dz] * size_y + ys[dy]

    def behind(offset):
        dx, dy, dz = offset
        return ahead(((size_x - dx) % size_x, (size_y - dy) % size_y, (size_z - dz) % size_z))

    partner = (me_x, me_dev + 1 - 2 * core)
    barrier = pltpu.get_barrier_semaphore()

    loads = [
        pltpu.make_async_copy(source, target, load_sem.at[index])
        for index, (source, target) in enumerate(zip(inputs, loaded, strict=True))
    ]
    for load in loads:
        load.start()
    for block in range(chips // 8):
        recv_buf[pl.ds(block * 64 + FIELDS, 8, stride=8), :] = jnp.zeros((8, LANES), F32)

    pl.semaphore_signal(barrier, inc=1, device_id=partner, device_id_type=MESH)
    for offset in near:
        x, zy = ahead(offset)
        pl.semaphore_signal(barrier, inc=1, device_id=(x, zy * CORES + core), device_id_type=MESH)

    source_ref, slot_ref, owner_ref, counts_ref, partials_ref, residual_ref, weight_ref, prior_ref = loaded
    for load in loads:
        load.wait()

    for block in range(chips // 8):
        rows = pl.ds(block * 8, 8)
        root = jnp.sqrt(weight_ref[rows, :])
        cell = (source_ref[rows, :] * LANES + slot_ref[rows, :]).astype(F32)
        send_buf[pl.ds(block * 64 + PARAMS, 8, stride=8), :] = residual_ref[rows, :] * root
        send_buf[pl.ds(block * 64 + PARAMS + 1, 8, stride=8), :] = cell
        for row in range(8):
            tile = block * 8 + row
            send_buf[tile * 8 : tile * 8 + PARAMS, :] = (
                partials_ref[:, tile * LANES : (tile + 1) * LANES] * root[row : row + 1, :]
            )
    facts[pl.ds(pl.multiple_of(core * 8, 8), 8), :] = jnp.concatenate(
        [prior_ref[...], counts_ref[...].astype(F32), jnp.zeros((2, LANES), F32)], axis=0
    )

    pl.semaphore_wait(barrier, len(near) + 1)
    for offset in vouchers:
        x, zy = behind(offset)
        pl.semaphore_signal(vouched, inc=1, device_id=(x, zy * CORES + core), device_id_type=MESH)

    facts_copy = pltpu.make_async_remote_copy(
        src_ref=facts.at[pl.ds(pl.multiple_of(core * 8, 8), 8), :],
        dst_ref=facts.at[pl.ds(pl.multiple_of(core * 8, 8), 8), :],
        send_sem=pair_send.at[0],
        recv_sem=pair_recv.at[0],
        device_id=partner,
        device_id_type=MESH,
    )
    facts_copy.start()

    def send_tile(slot):
        x, zy = ahead(offsets[slot])
        chip = x * (size_z * size_y) + zy
        pltpu.make_async_remote_copy(
            src_ref=send_buf.at[pl.ds(pl.multiple_of(chip * 8, 8), FIELDS), :],
            dst_ref=recv_buf.at[pl.ds(slot * 8, FIELDS), :],
            send_sem=send_sem,
            recv_sem=recv_sem.at[slot // GROUP],
            device_id=(x, zy * CORES + core),
            device_id_type=MESH,
        ).start()

    for slot in nearby:
        send_tile(slot)
    pl.semaphore_wait(vouched, len(vouchers))
    for slot in beyond:
        send_tile(slot)
    recv_buf[(chips - 1) * 8 : chips * 8 - 1, :] = send_buf[pl.ds(pl.multiple_of(me_chip * 8, 8), 8), :][0:FIELDS, :]

    sublane = lax.broadcasted_iota(jnp.int32, (LANES, LANES), 0)
    lane = lax.broadcasted_iota(jnp.int32, (1, LANES), 1)
    for side in range(CORES):
        base = (me_chip * CORES + side) * LANES

        def look(step, found):
            rows = owner_ref[pl.ds(pl.multiple_of(step * 8, 8), 8), :] - base
            for row in range(8):
                here = lane + (step * 8 + row) * LANES
                found = jnp.where(rows[row : row + 1, :] == sublane, here, found)
            return found

        found = lax.fori_loop(0, owner_ref.shape[0] // 8, look, jnp.zeros((LANES, LANES), jnp.int32))
        first = jnp.sum(found.astype(F32), axis=1, keepdims=True)
        table[side, 0] = jnp.broadcast_to(first, (LANES, LANES)).astype(jnp.int32).astype(jnp.int16)

    facts_copy.wait()
    for side in range(CORES):
        count = column_of(facts[side * 8 + PARAMS : side * 8 + PARAMS + 1, :])
        table[side, 1] = jnp.broadcast_to(count, (LANES, LANES)).astype(jnp.int32).astype(jnp.int16)

    def wait_rows(source, target, count, send, recv, to):
        return pltpu.make_async_remote_copy(
            src_ref=source.at[pl.ds(0, count)],
            dst_ref=target.at[pl.ds(0, count)],
            send_sem=send,
            recv_sem=recv,
            device_id=to,
            device_id_type=MESH,
        )

    low = lax.broadcasted_iota(jnp.int32, (8, LANES), 1) < LANES // 2
    total[...] = jnp.zeros_like(total)

    def gather_group(q):
        sides = ([], [])
        for v in range(GROUP // 2):
            start = (q * GROUP + v * 2) * 8
            even = recv_buf[start : start + 8, :]
            odd = recv_buf[start + 8 : start + 16, :]
            sides[0].append(jnp.where(low, even, pltpu.roll(odd, LANES // 2, 1)))
            sides[1].append(jnp.where(low, pltpu.roll(even, LANES // 2, 1), odd))
        for side in range(CORES):
            sources, slots, terms_of, picked_of = [], [], [], [[] for _ in range(GROUP // 2)]
            for v, rows in enumerate(sides[side]):
                place = (q * (GROUP // 2) + v) * 8
                halves[side, place : place + 8, :] = rows
                cell = jnp.broadcast_to(rows[FIELDS - 1 : FIELDS, :], (PACK, LANES)).astype(jnp.int32)
                sources.append((cell // LANES).astype(jnp.int16))
                slots.append((cell % LANES).astype(jnp.int16))
                terms = jnp.concatenate([rows[i : i + 1, :] * rows for i in range(PARAMS)], axis=0)
                parts = jnp.concatenate([*split_bf16(terms), jnp.zeros((8, LANES), F32)], axis=0)
                terms_of.append(parts.astype(BF16))
            for part in range(LANES // PACK):
                picked = slice(part * PACK, (part + 1) * PACK)
                source, count = table[side, 0, picked, :], table[side, 1, picked, :]
                for v in range(GROUP // 2):
                    inside = (sources[v] == source) & (slots[v] < count)
                    mark = jnp.where(inside, jnp.ones((PACK, LANES), BF16), jnp.zeros((PACK, LANES), BF16))
                    onehot[side, picked, q * WIDE + v * LANES : q * WIDE + (v + 1) * LANES] = mark.astype(F8)
                    picked_of[v].append(mark)
            total[side] += lax.dot_general(
                jnp.concatenate(terms_of, axis=1),
                jnp.concatenate([jnp.concatenate(marks, axis=0) for marks in picked_of], axis=1),
                (((1,), (1,)), ((), ())),
                preferred_element_type=F32,
            )

    order = list(range(groups))
    for q in order:
        count = GROUP - 1 if q == groups - 1 else GROUP
        wait_rows(send_buf, recv_buf, count * FIELDS, send_sem, recv_sem.at[q], partner).wait_recv()
        gather_group(q)

    span = PARAMS * 8
    for side in range(CORES):
        sums[side * span : (side + 1) * span, :] = (
            total[side, 0:span, :] + total[side, span : 2 * span, :] + total[side, 2 * span : 3 * span, :]
        )
    sums_copy = pltpu.make_async_remote_copy(
        src_ref=sums,
        dst_ref=other_sums,
        send_sem=pair_send.at[1],
        recv_sem=pair_recv.at[1],
        device_id=partner,
        device_id_type=MESH,
    )
    sums_copy.start()
    sums_copy.wait_recv()

    def summed(row):
        rows = pl.ds(row, CORES, stride=span)
        return sums[rows, :] + other_sums[rows, :]

    normal = [[None] * PARAMS for _ in range(PARAMS)]
    for i in range(PARAMS):
        for j in range(i, PARAMS):
            entry = summed(i * 8 + j)
            if i == j:
                entry = entry + facts[pl.ds(i, CORES, stride=8), :]
            normal[i][j] = entry
            normal[j][i] = entry
    moments = [summed(i * 8 + PARAMS) for i in range(PARAMS)]
    updates = solve_blocks(normal, moments)
    for i in range(PARAMS):
        update_rows[pl.ds(i, CORES, stride=8), :] = updates[i]
    update_rows[pl.ds(PARAMS, CORES, stride=8), :] = jnp.full((CORES, LANES), -1.0, F32)
    for row in (PARAMS + 1, PARAMS + 2):
        update_rows[pl.ds(row, CORES, stride=8), :] = jnp.zeros((CORES, LANES), F32)
    updates_ref[...] = update_rows[pl.ds(pl.multiple_of(core * 8, 8), 8), :][0:PARAMS, :]

    spread = []
    for side in range(CORES):
        parts = split_bf16(update_rows[side * 8 : side * 8 + 8, :])
        spread.append(jnp.concatenate([*parts, jnp.zeros((8, LANES), F32)], axis=0).astype(BF16))

    squares = jnp.zeros((1, LANES), F32)
    for q in range(groups):
        fitted = []
        for side in range(CORES):
            got = lax.dot_general(
                spread[side],
                onehot[side, :, q * WIDE : (q + 1) * WIDE],
                (((1,), (0,)), ((), ())),
                preferred_element_type=F32,
            )
            fitted.append(got[0:8, :] + got[8:16, :] + got[16:24, :])
        for v in range(GROUP // 2):
            fresh = []
            for side in range(CORES):
                rows = halves[side, (q * GROUP // 2 + v) * 8 : (q * GROUP // 2 + v + 1) * 8, :]
                term = rows * fitted[side][:, v * LANES : (v + 1) * LANES]
                line = -jnp.sum(term, axis=0, keepdims=True)
                squares = squares + line * line
                fresh.append(line)
            left, right = fresh
            at = q * GROUP + v * 2
            fresh_out[at, 0:1] = jnp.where(low[0:1], left, pltpu.roll(right, LANES // 2, 1))
            fresh_out[at + 1, 0:1] = jnp.where(low[0:1], pltpu.roll(left, LANES // 2, 1), right)
    count_row = counts_ref[...].astype(F32)
    squares = squares + pltpu.roll(squares, LANES // 2, 1)
    count_row = count_row + pltpu.roll(count_row, LANES // 2, 1)
    square_row = jnp.where(low[0:1], squares, count_row)
    for slot in range(chips):
        fresh_out[slot, 1:2] = square_row

    def send_fresh(slot):
        x, zy = behind(offsets[slot])
        pltpu.make_async_remote_copy(
            src_ref=fresh_out.at[slot],
            dst_ref=fresh_in.at[me_chip],
            send_sem=back_send,
            recv_sem=back_recv,
            device_id=(x, zy * CORES + core),
            device_id_type=MESH,
        ).start()

    for slot in sorted(range(chips - 1), key=lambda slot: -hops(offsets[slot], shape)):
        send_fresh(slot)
    fresh_in[me_chip] = fresh_out[chips - 1]
    wait_rows(fresh_in, fresh_in, chips - 1, back_send, back_recv, partner).wait_recv()
    squares_mine[...] = jnp.sum(fresh_in[:, 1, :], axis=0, keepdims=True)
    square_copy = pltpu.make_async_remote_copy(
        src_ref=squares_mine,
        dst_ref=squares_other,
        send_sem=pair_send.at[2],
        recv_sem=pair_recv.at[2],
        device_id=partner,
        device_id_type=MESH,
    )
    square_copy.start()
    fresh = fresh_in[:, 0, :]
    square_copy.wait_recv()
    whole = squares_mine[...] + squares_other[...]
    square_sum = jnp.sum(jnp.where(low[0:1], whole, 0.0), axis=1, keepdims=True)
    count_sum = jnp.sum(jnp.where(low[0:1], 0.0, whole), axis=1, keepdims=True)
    norm = jnp.sqrt(square_sum / count_sum + 1e-6)
    norm_ref[...] = jnp.broadcast_to(norm, (1, LANES))
    standard_ref[...] = fresh / norm

    wait_rows(send_buf, recv_buf, (chips - 1) * FIELDS, send_sem, send_sem, partner).wait_send()
    sums_copy.wait_send()
    square_copy.wait_send()
    wait_rows(fresh_in, fresh_in, chips - 1, back_send, back_recv, partner).wait_send()


def finish(*refs):
    copies = [
        pltpu.make_async_copy(source, target, refs[6].at[index])
        for index, (source, target) in enumerate(zip(refs[0:3], refs[3:6], strict=True))
    ]
    for copy in copies:
        copy.start()
    for copy in copies:
        copy.wait()


def body(shape, source_id, slot, owner, counts, partials, residual, weight, prior):
    size_x, size_y, size_z = shape
    chips = size_x * size_y * size_z
    groups = chips // GROUP
    square = (chips, LANES)
    arrays = (
        source_id.reshape(square),
        slot.reshape(square),
        owner.reshape(-1, LANES),
        counts.reshape(1, LANES),
        partials,
        residual.reshape(square),
        weight.reshape(square),
        prior,
    )
    vmem = pl.BlockSpec(memory_space=pltpu.VMEM)
    results = (
        jax.ShapeDtypeStruct((PARAMS, LANES), F32),
        jax.ShapeDtypeStruct(square, F32),
        jax.ShapeDtypeStruct((1, LANES), F32),
    )
    exchanged = pl.pallas_call(
        functools.partial(kernel, shape),
        out_shape=tuple(pltpu.VMEM(result.shape, result.dtype) for result in results),
        in_specs=[pl.BlockSpec(memory_space=pl.ANY)] * 8,
        out_specs=(vmem, vmem, vmem),
        scratch_shapes=[pltpu.VMEM(array.shape, array.dtype) for array in arrays]
        + [
            pltpu.VMEM((chips * 8, LANES), F32),
            pltpu.VMEM((chips * 8, LANES), F32),
            pltpu.VMEM((CORES, chips * 4, LANES), F32),
            pltpu.VMEM((CORES, LANES, chips * LANES // 2), F8),
            pltpu.VMEM((CORES, LANES, LANES), F32),
            pltpu.VMEM((CORES, 2, LANES, LANES), jnp.int16),
            pltpu.VMEM((CORES * 8, LANES), F32),
            pltpu.VMEM((CORES * PARAMS * 8, LANES), F32),
            pltpu.VMEM((CORES * PARAMS * 8, LANES), F32),
            pltpu.VMEM((CORES * 8, LANES), F32),
            pltpu.VMEM((chips, 2, LANES), F32),
            pltpu.VMEM((chips, 2, LANES), F32),
            pltpu.VMEM((1, LANES), F32),
            pltpu.VMEM((1, LANES), F32),
            pltpu.SemaphoreType.DMA((8,)),
            pltpu.SemaphoreType.DMA,
            pltpu.SemaphoreType.DMA((groups,)),
            pltpu.SemaphoreType.DMA((3,)),
            pltpu.SemaphoreType.DMA((3,)),
            pltpu.SemaphoreType.DMA,
            pltpu.SemaphoreType.DMA,
            pltpu.SemaphoreType.REGULAR,
        ],
        compiler_params=pltpu.CompilerParams(collective_id=0, has_side_effects=True),
    )(*arrays)
    place = pl.BlockSpec(memory_space=pl.ANY)
    updates, standard, norm = pl.pallas_call(
        finish,
        out_shape=results,
        in_specs=[place] * 3,
        out_specs=(place, place, place),
        scratch_shapes=[pltpu.SemaphoreType.DMA((3,))],
    )(*(pltpu.with_memory_space_constraint(value, pltpu.VMEM) for value in exchanged))
    return updates, standard.reshape(-1), norm[0, 0]


def solution(mesh):
    shape = (mesh.shape["grp"], ROWS_Y, mesh.shape["dev"] // (ROWS_Y * CORES))
    rows = P(("grp", "dev"))
    columns = P(None, ("grp", "dev"))
    in_specs = (rows, rows, P(), rows, columns, rows, rows, columns)
    out_specs = (columns, rows, P())
    return jax.shard_map(
        functools.partial(body, shape), mesh=mesh, in_specs=in_specs, out_specs=out_specs, check_vma=False
    )
```

```python
import functools

import jax
import jax.numpy as jnp
from jax import lax
from jax.experimental import pallas as pl
from jax.experimental.pallas import tpu as pltpu
from jax.sharding import PartitionSpec as P

MESH = pl.DeviceIdType.MESH
F32 = jnp.float32
BF16 = jnp.bfloat16
F8 = jnp.float8_e4m3fn
LANES = 128
ROWS_Y = 4
CORES = 2
PARAMS = 5
FIELDS = 7
GROUP = 16
WIDE = GROUP // 2 * LANES
PACK = 16


def split_bf16(value):
    high = value.astype(BF16).astype(F32)
    rest = value - high
    middle = rest.astype(BF16).astype(F32)
    return high, middle, rest - middle


def column_of(row):
    square = (LANES, LANES)
    diagonal = lax.broadcasted_iota(jnp.int32, square, 0) == lax.broadcasted_iota(jnp.int32, square, 1)
    return jnp.sum(jnp.where(diagonal, jnp.broadcast_to(row, square), 0.0), axis=1, keepdims=True)


def solve_blocks(normal, moments):
    params = len(moments)
    factor = {}
    for column in range(params):
        running = normal[column][column]
        for earlier in range(column):
            running = running - factor[column, earlier] ** 2
        pivot_value = jnp.sqrt(running)
        factor[column, column] = pivot_value
        for target in range(column + 1, params):
            current = normal[target][column]
            for earlier in range(column):
                current = current - factor[target, earlier] * factor[column, earlier]
            factor[target, column] = current / pivot_value
    forward = []
    for target in range(params):
        current = moments[target]
        for earlier in range(target):
            current = current - factor[target, earlier] * forward[earlier]
        forward.append(current / factor[target, target])
    backward = [None] * params
    for target in reversed(range(params)):
        current = forward[target]
        for later in range(target + 1, params):
            current = current - factor[later, target] * backward[later]
        backward[target] = current / factor[target, target]
    return backward


def hops(offset, shape):
    return sum(min(step, size - step) for step, size in zip(offset, shape, strict=True))


def send_order(shape):
    size_x, size_y, size_z = shape
    reach = size_z // 4
    every = [(x, y, z) for y in range(size_y) for z in range(size_z) for x in range(size_x)]
    every.sort(key=lambda offset: -hops(offset, shape))
    near = [offset for offset in every[:-1] if min(offset[2], size_z - offset[2]) <= reach]
    far = [offset for offset in every[:-1] if offset not in near]
    return near, far, [(0, 0, reach), (0, 0, size_z - reach)]


def kernel(
    shape,
    *refs,
):
    inputs, (updates_ref, standard_ref, norm_ref) = refs[0:8], refs[8:11]
    loaded = refs[11:19]
    (send_buf, recv_buf, halves, onehot, total, table, facts, sums, other_sums) = refs[19:28]
    (update_rows, fresh_out, fresh_in, squares_mine, squares_other) = refs[28:33]
    (load_sem, send_sem, recv_sem, pair_send, pair_recv, back_send, back_recv, vouched) = refs[33:41]
    size_x, size_y, size_z = shape
    chips = size_x * size_y * size_z
    groups = chips // GROUP
    me_x = lax.axis_index("grp")
    me_dev = lax.axis_index("dev")
    core = me_dev % CORES
    me_y = (me_dev // CORES) % size_y
    me_z = me_dev // (CORES * size_y)
    me_chip = (me_x * size_z + me_z) * size_y + me_y


    xs = [(me_x + dx) % size_x for dx in range(size_x)]
    ys = [(me_y + dy) % size_y for dy in range(size_y)]
    zs = [(me_z + dz) % size_z for dz in range(size_z)]
    near, far, vouchers = send_order(shape)
    own = len(near)
    offsets = near + [(0, 0, 0)] + far
    nearby, beyond = range(own), range(own + 1, chips)

    def ahead(offset):
        dx, dy, dz = offset
        return xs[dx], zs[dz] * size_y + ys[dy]

    def behind(offset):
        dx, dy, dz = offset
        return ahead(((size_x - dx) % size_x, (size_y - dy) % size_y, (size_z - dz) % size_z))

    partner = (me_x, me_dev + 1 - 2 * core)
    barrier = pltpu.get_barrier_semaphore()

    loads = [
        pltpu.make_async_copy(source, target, load_sem.at[index])
        for index, (source, target) in enumerate(zip(inputs, loaded, strict=True))
    ]
    for load in loads:
        load.start()
    for block in range(chips // 8):
        recv_buf[pl.ds(block * 64 + FIELDS, 8, stride=8), :] = jnp.zeros((8, LANES), F32)

    pl.semaphore_signal(barrier, inc=1, device_id=partner, device_id_type=MESH)
    for offset in near:
        x, zy = ahead(offset)
        pl.semaphore_signal(barrier, inc=1, device_id=(x, zy * CORES + core), device_id_type=MESH)

    source_ref, slot_ref, owner_ref, counts_ref, partials_ref, residual_ref, weight_ref, prior_ref = loaded
    for load in loads:
        load.wait()

    for block in range(chips // 8):
        rows = pl.ds(block * 8, 8)
        root = jnp.sqrt(weight_ref[rows, :])
        cell = (source_ref[rows, :] * LANES + slot_ref[rows, :]).astype(F32)
        send_buf[pl.ds(block * 64 + PARAMS, 8, stride=8), :] = residual_ref[rows, :] * root
        send_buf[pl.ds(block * 64 + PARAMS + 1, 8, stride=8), :] = cell
        for row in range(8):
            tile = block * 8 + row
            send_buf[tile * 8 : tile * 8 + PARAMS, :] = (
                partials_ref[:, tile * LANES : (tile + 1) * LANES] * root[row : row + 1, :]
            )
    facts[pl.ds(pl.multiple_of(core * 8, 8), 8), :] = jnp.concatenate(
        [prior_ref[...], counts_ref[...].astype(F32), jnp.zeros((2, LANES), F32)], axis=0
    )

    pl.semaphore_wait(barrier, len(near) + 1)
    for offset in vouchers:
        x, zy = behind(offset)
        pl.semaphore_signal(vouched, inc=1, device_id=(x, zy * CORES + core), device_id_type=MESH)

    facts_copy = pltpu.make_async_remote_copy(
        src_ref=facts.at[pl.ds(pl.multiple_of(core * 8, 8), 8), :],
        dst_ref=facts.at[pl.ds(pl.multiple_of(core * 8, 8), 8), :],
        send_sem=pair_send.at[0],
        recv_sem=pair_recv.at[0],
        device_id=partner,
        device_id_type=MESH,
    )
    facts_copy.start()

    def send_tile(slot):
        x, zy = ahead(offsets[slot])
        chip = x * (size_z * size_y) + zy
        pltpu.make_async_remote_copy(
            src_ref=send_buf.at[pl.ds(pl.multiple_of(chip * 8, 8), FIELDS), :],
            dst_ref=recv_buf.at[pl.ds(slot * 8, FIELDS), :],
            send_sem=send_sem,
            recv_sem=recv_sem.at[slot // GROUP],
            device_id=(x, zy * CORES + core),
            device_id_type=MESH,
        ).start()

    for slot in nearby:
        send_tile(slot)
    pl.semaphore_wait(vouched, len(vouchers))
    for slot in beyond:
        send_tile(slot)
    recv_buf[own * 8 : own * 8 + FIELDS, :] = send_buf[pl.ds(pl.multiple_of(me_chip * 8, 8), 8), :][0:FIELDS, :]

    sublane = lax.broadcasted_iota(jnp.int32, (LANES, LANES), 0)
    lane = lax.broadcasted_iota(jnp.int32, (1, LANES), 1)
    for side in range(CORES):
        base = (me_chip * CORES + side) * LANES

        def look(step, found):
            rows = owner_ref[pl.ds(pl.multiple_of(step * 8, 8), 8), :] - base
            for row in range(8):
                here = lane + (step * 8 + row) * LANES
                found = jnp.where(rows[row : row + 1, :] == sublane, here, found)
            return found

        found = lax.fori_loop(0, owner_ref.shape[0] // 8, look, jnp.zeros((LANES, LANES), jnp.int32))
        first = jnp.sum(found.astype(F32), axis=1, keepdims=True)
        table[side, 0] = jnp.broadcast_to(first, (LANES, LANES)).astype(jnp.int32).astype(jnp.int16)

    facts_copy.wait()
    for side in range(CORES):
        count = column_of(facts[side * 8 + PARAMS : side * 8 + PARAMS + 1, :])
        table[side, 1] = jnp.broadcast_to(count, (LANES, LANES)).astype(jnp.int32).astype(jnp.int16)

    def wait_rows(source, target, count, send, recv, to):
        return pltpu.make_async_remote_copy(
            src_ref=source.at[pl.ds(0, count)],
            dst_ref=target.at[pl.ds(0, count)],
            send_sem=send,
            recv_sem=recv,
            device_id=to,
            device_id_type=MESH,
        )

    low = lax.broadcasted_iota(jnp.int32, (8, LANES), 1) < LANES // 2
    total[...] = jnp.zeros_like(total)

    def gather_group(q):
        sides = ([], [])
        for v in range(GROUP // 2):
            start = (q * GROUP + v * 2) * 8
            even = recv_buf[start : start + 8, :]
            odd = recv_buf[start + 8 : start + 16, :]
            sides[0].append(jnp.where(low, even, pltpu.roll(odd, LANES // 2, 1)))
            sides[1].append(jnp.where(low, pltpu.roll(even, LANES // 2, 1), odd))
        for side in range(CORES):
            sources, slots, terms_of, picked_of = [], [], [], [[] for _ in range(GROUP // 2)]
            for v, rows in enumerate(sides[side]):
                place = (q * (GROUP // 2) + v) * 8
                halves[side, place : place + 8, :] = rows
                cell = jnp.broadcast_to(rows[FIELDS - 1 : FIELDS, :], (PACK, LANES)).astype(jnp.int32)
                sources.append((cell // LANES).astype(jnp.int16))
                slots.append((cell % LANES).astype(jnp.int16))
                terms = jnp.concatenate([rows[i : i + 1, :] * rows for i in range(PARAMS)], axis=0)
                parts = jnp.concatenate([*split_bf16(terms), jnp.zeros((8, LANES), F32)], axis=0)
                terms_of.append(parts.astype(BF16))
            for part in range(LANES // PACK):
                picked = slice(part * PACK, (part + 1) * PACK)
                source, count = table[side, 0, picked, :], table[side, 1, picked, :]
                for v in range(GROUP // 2):
                    inside = (sources[v] == source) & (slots[v] < count)
                    mark = jnp.where(inside, jnp.ones((PACK, LANES), BF16), jnp.zeros((PACK, LANES), BF16))
                    onehot[side, picked, q * WIDE + v * LANES : q * WIDE + (v + 1) * LANES] = mark.astype(F8)
                    picked_of[v].append(mark)
            total[side] += lax.dot_general(
                jnp.concatenate(terms_of, axis=1),
                jnp.concatenate([jnp.concatenate(marks, axis=0) for marks in picked_of], axis=1),
                (((1,), (1,)), ((), ())),
                preferred_element_type=F32,
            )

    order = list(range(groups))
    for q in order:
        count = GROUP - 1 if q == own // GROUP else GROUP
        wait_rows(send_buf, recv_buf, count * FIELDS, send_sem, recv_sem.at[q], partner).wait_recv()
        gather_group(q)

    span = PARAMS * 8
    for side in range(CORES):
        sums[side * span : (side + 1) * span, :] = (
            total[side, 0:span, :] + total[side, span : 2 * span, :] + total[side, 2 * span : 3 * span, :]
        )
    sums_copy = pltpu.make_async_remote_copy(
        src_ref=sums,
        dst_ref=other_sums,
        send_sem=pair_send.at[1],
        recv_sem=pair_recv.at[1],
        device_id=partner,
        device_id_type=MESH,
    )
    sums_copy.start()
    sums_copy.wait_recv()

    def summed(row):
        rows = pl.ds(row, CORES, stride=span)
        return sums[rows, :] + other_sums[rows, :]

    normal = [[None] * PARAMS for _ in range(PARAMS)]
    for i in range(PARAMS):
        for j in range(i, PARAMS):
            entry = summed(i * 8 + j)
            if i == j:
                entry = entry + facts[pl.ds(i, CORES, stride=8), :]
            normal[i][j] = entry
            normal[j][i] = entry
    moments = [summed(i * 8 + PARAMS) for i in range(PARAMS)]
    updates = solve_blocks(normal, moments)
    for i in range(PARAMS):
        update_rows[pl.ds(i, CORES, stride=8), :] = updates[i]
    update_rows[pl.ds(PARAMS, CORES, stride=8), :] = jnp.full((CORES, LANES), -1.0, F32)
    for row in (PARAMS + 1, PARAMS + 2):
        update_rows[pl.ds(row, CORES, stride=8), :] = jnp.zeros((CORES, LANES), F32)
    updates_ref[...] = update_rows[pl.ds(pl.multiple_of(core * 8, 8), 8), :][0:PARAMS, :]

    spread = []
    for side in range(CORES):
        parts = split_bf16(update_rows[side * 8 : side * 8 + 8, :])
        spread.append(jnp.concatenate([*parts, jnp.zeros((8, LANES), F32)], axis=0).astype(BF16))

    squares = jnp.zeros((1, LANES), F32)
    for q in range(groups):
        fitted = []
        for side in range(CORES):
            got = lax.dot_general(
                spread[side],
                onehot[side, :, q * WIDE : (q + 1) * WIDE],
                (((1,), (0,)), ((), ())),
                preferred_element_type=F32,
            )
            fitted.append(got[0:8, :] + got[8:16, :] + got[16:24, :])
        for v in range(GROUP // 2):
            fresh = []
            for side in range(CORES):
                rows = halves[side, (q * GROUP // 2 + v) * 8 : (q * GROUP // 2 + v + 1) * 8, :]
                term = rows * fitted[side][:, v * LANES : (v + 1) * LANES]
                line = -jnp.sum(term, axis=0, keepdims=True)
                squares = squares + line * line
                fresh.append(line)
            left, right = fresh
            at = q * GROUP + v * 2
            fresh_out[at, 0:1] = jnp.where(low[0:1], left, pltpu.roll(right, LANES // 2, 1))
            fresh_out[at + 1, 0:1] = jnp.where(low[0:1], pltpu.roll(left, LANES // 2, 1), right)
    count_row = counts_ref[...].astype(F32)
    squares = squares + pltpu.roll(squares, LANES // 2, 1)
    count_row = count_row + pltpu.roll(count_row, LANES // 2, 1)
    square_row = jnp.where(low[0:1], squares, count_row)
    for slot in range(chips):
        fresh_out[slot, 1:2] = square_row

    def send_fresh(slot):
        x, zy = behind(offsets[slot])
        pltpu.make_async_remote_copy(
            src_ref=fresh_out.at[slot],
            dst_ref=fresh_in.at[me_chip],
            send_sem=back_send,
            recv_sem=back_recv,
            device_id=(x, zy * CORES + core),
            device_id_type=MESH,
        ).start()

    for slot in sorted([*nearby, *beyond], key=lambda slot: -hops(offsets[slot], shape)):
        send_fresh(slot)
    fresh_in[me_chip] = fresh_out[own]
    wait_rows(fresh_in, fresh_in, chips - 1, back_send, back_recv, partner).wait_recv()
    squares_mine[...] = jnp.sum(fresh_in[:, 1, :], axis=0, keepdims=True)
    square_copy = pltpu.make_async_remote_copy(
        src_ref=squares_mine,
        dst_ref=squares_other,
        send_sem=pair_send.at[2],
        recv_sem=pair_recv.at[2],
        device_id=partner,
        device_id_type=MESH,
    )
    square_copy.start()
    fresh = fresh_in[:, 0, :]
    square_copy.wait_recv()
    whole = squares_mine[...] + squares_other[...]
    square_sum = jnp.sum(jnp.where(low[0:1], whole, 0.0), axis=1, keepdims=True)
    count_sum = jnp.sum(jnp.where(low[0:1], 0.0, whole), axis=1, keepdims=True)
    norm = jnp.sqrt(square_sum / count_sum + 1e-6)
    norm_ref[...] = jnp.broadcast_to(norm, (1, LANES))
    standard_ref[...] = fresh / norm

    wait_rows(send_buf, recv_buf, (chips - 1) * FIELDS, send_sem, send_sem, partner).wait_send()
    sums_copy.wait_send()
    square_copy.wait_send()
    wait_rows(fresh_in, fresh_in, chips - 1, back_send, back_recv, partner).wait_send()


def finish(*refs):
    copies = [
        pltpu.make_async_copy(source, target, refs[6].at[index])
        for index, (source, target) in enumerate(zip(refs[0:3], refs[3:6], strict=True))
    ]
    for copy in copies:
        copy.start()
    for copy in copies:
        copy.wait()


def body(shape, source_id, slot, owner, counts, partials, residual, weight, prior):
    size_x, size_y, size_z = shape
    chips = size_x * size_y * size_z
    groups = chips // GROUP
    square = (chips, LANES)
    arrays = (
        source_id.reshape(square),
        slot.reshape(square),
        owner.reshape(-1, LANES),
        counts.reshape(1, LANES),
        partials,
        residual.reshape(square),
        weight.reshape(square),
        prior,
    )
    vmem = pl.BlockSpec(memory_space=pltpu.VMEM)
    results = (
        jax.ShapeDtypeStruct((PARAMS, LANES), F32),
        jax.ShapeDtypeStruct(square, F32),
        jax.ShapeDtypeStruct((1, LANES), F32),
    )
    exchanged = pl.pallas_call(
        functools.partial(kernel, shape),
        out_shape=tuple(pltpu.VMEM(result.shape, result.dtype) for result in results),
        in_specs=[pl.BlockSpec(memory_space=pl.ANY)] * 8,
        out_specs=(vmem, vmem, vmem),
        scratch_shapes=[pltpu.VMEM(array.shape, array.dtype) for array in arrays]
        + [
            pltpu.VMEM((chips * 8, LANES), F32),
            pltpu.VMEM((chips * 8, LANES), F32),
            pltpu.VMEM((CORES, chips * 4, LANES), F32),
            pltpu.VMEM((CORES, LANES, chips * LANES // 2), F8),
            pltpu.VMEM((CORES, LANES, LANES), F32),
            pltpu.VMEM((CORES, 2, LANES, LANES), jnp.int16),
            pltpu.VMEM((CORES * 8, LANES), F32),
            pltpu.VMEM((CORES * PARAMS * 8, LANES), F32),
            pltpu.VMEM((CORES * PARAMS * 8, LANES), F32),
            pltpu.VMEM((CORES * 8, LANES), F32),
            pltpu.VMEM((chips, 2, LANES), F32),
            pltpu.VMEM((chips, 2, LANES), F32),
            pltpu.VMEM((1, LANES), F32),
            pltpu.VMEM((1, LANES), F32),
            pltpu.SemaphoreType.DMA((8,)),
            pltpu.SemaphoreType.DMA,
            pltpu.SemaphoreType.DMA((groups,)),
            pltpu.SemaphoreType.DMA((3,)),
            pltpu.SemaphoreType.DMA((3,)),
            pltpu.SemaphoreType.DMA,
            pltpu.SemaphoreType.DMA,
            pltpu.SemaphoreType.REGULAR,
        ],
        compiler_params=pltpu.CompilerParams(collective_id=0, has_side_effects=True),
    )(*arrays)
    place = pl.BlockSpec(memory_space=pl.ANY)
    updates, standard, norm = pl.pallas_call(
        finish,
        out_shape=results,
        in_specs=[place] * 3,
        out_specs=(place, place, place),
        scratch_shapes=[pltpu.SemaphoreType.DMA((3,))],
    )(*(pltpu.with_memory_space_constraint(value, pltpu.VMEM) for value in exchanged))
    return updates, standard.reshape(-1), norm[0, 0]


def solution(mesh):
    shape = (mesh.shape["grp"], ROWS_Y, mesh.shape["dev"] // (ROWS_Y * CORES))
    rows = P(("grp", "dev"))
    columns = P(None, ("grp", "dev"))
    in_specs = (rows, rows, P(), rows, columns, rows, rows, columns)
    out_specs = (columns, rows, P())
    return jax.shard_map(
        functools.partial(body, shape), mesh=mesh, in_specs=in_specs, out_specs=out_specs, check_vma=False
    )
```
